128 devices in a mesh: row: 8 (over x, core), col: 16 (over y, z).
Axes of the slice: x: 4, y: 4, z: 4, core: 2. Of those that a mesh axis runs over, the one named last changes fastest.
Arguments:
- panel_rows: float32 [8192, 4096], P('row', 'col'), may hold values from -0.75 to 0.75
- owner_slot: int32 [16, 16], replicated, may hold values from -1 to 31, as said below
Outputs:
- packed: float32 [8, 32, 512, 512], P('row', 'col')
The draws below stay inside these ranges and needn't reach their ends.
Inputs may be any that keep to these rules, and one draw needn't show every extreme that they name: For j <= i, owner_slot[i, j] is the position of tile (i, j) among the 32 positions of group i // 2; tiles of one group have distinct positions; entries above the diagonal are -1. Position p lies on the device of col index p // 2.
All inputs are finite; a program needn't handle non-finite values.
Results may differ from the reference program's by a relative error of at most 0.0003.
Values sent between devices are 32-bit elements; how exact they have to be, the bound alone decides.
No kernel may reach another device: no remote copies, remote signals or barrier semaphores. Data moves between devices by JAX's collectives and lax.ppermute only.
A program may use at most 128 MiB of HBM per device.

```python
import jax
import jax.numpy as jnp
from jax import lax

BLOCK = 512
K = 4096
ORDER = 8192
BR = 2
NB = 16
POS = 32
N_ROW = 8


def draw_owner_slot(key, part):
    groups = NB // BR
    block_row = jnp.arange(NB, dtype=jnp.int32)[:, None]
    block_col = jnp.arange(NB, dtype=jnp.int32)[None, :]
    row_keys = jax.random.split(jax.random.fold_in(key, 11), groups)
    orders = jax.vmap(lambda sub_key: jax.random.permutation(sub_key, POS))(row_keys).astype(jnp.int32)
    group_ids = jnp.arange(groups, dtype=jnp.int32)
    first_rows = group_ids * BR
    tile_total = BR * first_rows + BR * (BR + 1) // 2
    picked = jax.random.randint(jax.random.fold_in(key, 12), (groups,), 0, tile_total).astype(jnp.int32)
    top_place = jnp.argmax(orders == POS - 1, axis=1).astype(jnp.int32)
    offsets = top_place - picked
    row_group = block_row // BR
    first_own = row_group * BR
    index_in = (block_row * (block_row + 1) - first_own * (first_own + 1)) // 2 + block_col
    taken = (index_in + offsets[row_group[:, 0]][:, None]) % POS
    order_rows = orders[row_group[:, 0]]
    placed = jnp.take_along_axis(order_rows, taken, axis=1)
    return jnp.where(block_col <= block_row, placed, -1).astype(jnp.int32)


def levels(stream_key, extent, cuts, low, largest):
    level, own = 1.0, jax.random.fold_in(stream_key, 6)
    for dim, parts in cuts:
        draws = jnp.exp(jax.random.uniform(jax.random.fold_in(own, dim), (parts,), jnp.float32, low / len(cuts), largest / len(cuts)))
        level = level * jnp.repeat(draws, extent[dim] // parts).reshape([-1 if axis == dim else 1 for axis in range(len(extent))])
    return level


def noise(own_key, extent, width, bound, cuts=(), held_as=jnp.bfloat16):
    result = width * jax.random.normal(own_key, extent, jnp.float32)
    if cuts:
        result = result * levels(own_key, extent, cuts, -0.22, 0.18)
    return jnp.clip(result, -bound, bound).astype(held_as)


def setup_inputs(seed: int = 0) -> dict:
    key_list = jax.random.split(jax.random.key(seed), 3)
    return {
        "panel_rows": noise(key_list[0], (ORDER, K), (K ** -0.25), 0.75, ((0, 8), (1, 16)), jnp.float32),
        "owner_slot": draw_owner_slot(jax.random.fold_in(key_list[2], 71), 0),
    }


def slot_table(owner_slot, group_id, positions, per_group):
    blocks = owner_slot.shape[0]
    block_row = jnp.arange(blocks, dtype=jnp.int32)[:, None]
    block_col = jnp.arange(blocks, dtype=jnp.int32)[None, :]
    inside = (block_row // per_group == group_id) & (block_col <= block_row)
    wanted = jnp.arange(positions, dtype=jnp.int32)[:, None, None]
    matched = inside[None] & (owner_slot[None] == wanted)
    is_live = jnp.any(matched, axis=(1, 2))
    left_block = jnp.sum(jnp.where(matched, block_row[None], 0), axis=(1, 2)).astype(jnp.int32)
    right_block = jnp.sum(jnp.where(matched, block_col[None], 0), axis=(1, 2)).astype(jnp.int32)
    return left_block, right_block, is_live


def reference(panel_rows, owner_slot):
    tiles_all = panel_rows.reshape(NB, BLOCK, K)

    def group_tiles(group_id):
        left_block, right_block, is_live = slot_table(owner_slot, group_id, POS, BR)

        def single(packed_item):
            left_one, right_one, flag = packed_item

            def compute():
                return lax.dot_general(tiles_all[left_one], tiles_all[right_one], (((1,), (1,)), ((), ())),
                                       precision=lax.Precision.HIGHEST, preferred_element_type=jnp.float32)

            def blank():
                return jnp.zeros((BLOCK, BLOCK), jnp.float32)

            return lax.cond(flag, compute, blank)

        return lax.map(single, (left_block, right_block, is_live))

    return lax.map(group_tiles, jnp.arange(N_ROW, dtype=jnp.int32))
```

```python
import functools

import jax
import jax.numpy as jnp
from jax import lax
from jax.experimental import pallas as pl
from jax.experimental.pallas import tpu as pltpu
from jax.sharding import Mesh
from jax.sharding import PartitionSpec as P


N = 4
VMEM = pltpu.VMEM
SMEM = pltpu.SMEM
GRANT = 60 * 1024 * 1024


def shift(value, axis, step):
    size = lax.axis_size(axis)
    return lax.ppermute(value, axis, [(k, (k + step) % size) for k in range(size)])


def specs(space, count):
    return [pl.BlockSpec(memory_space=space)] * count


def cut_kernel(q, at_ref, a_ref, own_ref, *sends):
    for kind in range(2):
        for step in range(N):
            part = lax.rem(at_ref[kind] + step, N)
            for block in range(2):
                start = pl.multiple_of((2 * block + kind) * N * q + part * q, q)
                piece = a_ref[pl.ds(start, q), :]
                if step == 0:
                    own_ref[kind, block * q : (block + 1) * q, :] = piece
                else:
                    sends[3 * kind + step - 1][block * q : (block + 1) * q, :] = piece


def cut(at, a):
    rows, inner = a.shape
    q = rows // 16
    piece = jax.ShapeDtypeStruct((2 * q, inner), a.dtype)
    return pl.pallas_call(
        functools.partial(cut_kernel, q),
        out_shape=[jax.ShapeDtypeStruct((2, 2 * q, inner), a.dtype)] + [piece] * 6,
        in_specs=specs(SMEM, 1) + specs(VMEM, 1),
        out_specs=specs(VMEM, 7),
        cost_estimate=pl.CostEstimate(flops=10**6, bytes_accessed=2 * rows * inner * 4, transcendentals=0),
        name="cut",
    )(at, a)


def product_kernel(q, kind, tab_ref, *refs):
    slabs, firsts, rests = refs[:4], refs[4:12], refs[12:20]
    outs, (a3, b3, acc) = refs[20:27], refs[27:]
    rows, inner = slabs[0].shape
    half = rows // 2

    def halves(value):
        high = value.astype(jnp.bfloat16)
        return high, (value - high.astype(jnp.float32)).astype(jnp.bfloat16)

    for s in range(N):
        col = 3 * s * inner
        high, low = halves(slabs[s][...])
        a3[:, col : col + inner] = high
        a3[:, col + inner : col + 2 * inner] = low
        a3[:, col + 2 * inner : col + 3 * inner] = high
        for k in range(8):
            high, low = halves(firsts[k][0] if s == 0 else rests[k][s - 1])
            at = slice(2 * q * k, 2 * q * (k + 1))
            b3[at, col : col + inner] = high
            b3[at, col + inner : col + 2 * inner] = high
            b3[at, col + 2 * inner : col + 3 * inner] = low

    part = half // 2

    def multiply(m, carry):
        start = pl.multiple_of(m * half, half)
        left = b3[pl.ds(start, half), :]
        for n in range(4):
            acc[n // 2, pl.ds(start, half), (n % 2) * part : (n % 2 + 1) * part] = lax.dot_general(
                left,
                a3[n * part : (n + 1) * part, :],
                (((1,), (1,)), ((), ())),
                preferred_element_type=jnp.float32,
            )
        return carry

    lax.fori_loop(0, 2, multiply, 0)

    own, d1a, d1b, d2a, d2b, d3a, d3b = outs
    places = [(own, k) for k in range(8)]
    for first, second in ((d1a, d1b), (d2a, d2b), (d3a, d3b)):
        places += [(first, k) for k in range(4)] + [(second, k) for k in range(4)]
    for index, (ref, place) in enumerate(places):
        code = tab_ref[kind, index]
        safe = jnp.maximum(code, 0)
        start = pl.multiple_of((safe // 2) * q, q)
        tile = acc[safe % 2, pl.ds(start, q), :]
        ref[place] = jnp.where(code >= 0, tile, 0.0)


def product(kind, tab, slabs, firsts, rests):
    rows, inner = slabs[0].shape
    q, half = rows // 16, rows // 2
    whole = lambda: pl.BlockSpec((rows, inner), lambda i: (0, 0))
    out = lambda n: jax.ShapeDtypeStruct((n, q, half), jnp.float32)
    out_spec = lambda n: pl.BlockSpec((n, q, half), lambda i: (0, 0, 0))
    counts = [8] + [4] * 6
    return pl.pallas_call(
        functools.partial(product_kernel, q, kind),
        grid=(1,),
        out_shape=[out(n) for n in counts],
        in_specs=specs(SMEM, 1)
        + [whole() for _ in range(4)]
        + [pl.BlockSpec((1, 2 * q, inner), lambda i: (kind, 0, 0)) for _ in range(8)]
        + [pl.BlockSpec((3, 2 * q, inner), lambda i: (kind, 0, 0)) for _ in range(8)],
        out_specs=[out_spec(n) for n in counts],
        scratch_shapes=[
            VMEM((rows, 12 * inner), jnp.bfloat16),
            VMEM((rows, 12 * inner), jnp.bfloat16),
            VMEM((2, rows, half), jnp.float32),
        ],
        compiler_params=pltpu.CompilerParams(vmem_limit_bytes=GRANT),
        cost_estimate=pl.CostEstimate(
            flops=2 * rows * rows * 12 * inner, bytes_accessed=12 * rows * inner * 4, transcendentals=0
        ),
        name="product",
    )(tab, *slabs, *firsts, *rests)


def sum_along(axis, parts):
    own, d1a, d1b, d2a, d2b, d3a, d3b = parts
    up_far = shift(d2a, axis, 1)
    down_far = shift(d2b, axis, -1)
    up_near = shift(d1b, axis, 1)
    down_near = shift(d3a, axis, -1)
    up = shift(d1a + up_far, axis, 1)
    down = shift(d3b + down_far, axis, -1)
    return [
        own[0:2] + up[0:2] + down_near[0:2],
        own[2:4] + up[2:4] + down_near[2:4],
        own[4:6] + down[0:2] + up_near[0:2],
        own[6:8] + down[2:4] + up_near[2:4],
    ]


def join_kernel(q, at_ref, *refs):
    pieces, out_ref, held = refs[:8], refs[8], refs[9]
    for kind in range(2):
        for step in range(N):
            part = lax.rem(at_ref[kind] + N - step, N)
            start = pl.multiple_of(kind * N * q + part * q, q)
            for slot in range(2):
                held[slot, pl.ds(start, q), :] = pieces[4 * kind + step][slot]
    for slot in range(2):
        out_ref[0, slot] = held[slot].T


def join(at, pieces):
    _, q, half = pieces[0].shape
    return pl.pallas_call(
        functools.partial(join_kernel, q),
        out_shape=jax.ShapeDtypeStruct((1, 2, half, half), jnp.float32),
        in_specs=specs(SMEM, 1) + specs(VMEM, 8),
        out_specs=pl.BlockSpec(memory_space=VMEM),
        scratch_shapes=[VMEM((2, half, half), jnp.float32)],
        compiler_params=pltpu.CompilerParams(vmem_limit_bytes=32 * 1024 * 1024),
        cost_estimate=pl.CostEstimate(flops=10**6, bytes_accessed=16 * half * half, transcendentals=0),
        name="join",
    )(at, *pieces)


def tile_codes(owner, x, c, y, z):
    blocks = owner.shape[0]
    i = lax.broadcasted_iota(jnp.int32, (blocks, blocks), 0)
    j = lax.broadcasted_iota(jnp.int32, (blocks, blocks), 1)
    group = j // 2
    other = jnp.where(group % 2 == c, 0, 1)
    array = other * 4 + (x - group // 2 + N) % N
    code = (array * 2 + j % 2) * 2 + i % 2 + 1
    code = jnp.where((i // 2 == 2 * x + c) & (j <= i), code, 0)
    far = jnp.arange(32, dtype=jnp.int32) // 8
    near = (jnp.arange(32, dtype=jnp.int32) // 2) % 4
    slot = jnp.arange(32, dtype=jnp.int32) % 2
    wanted = jnp.stack(
        [((y + far) % N) * 8 + ((z + near) % N) * 2 + slot, ((y + near) % N) * 8 + ((z + far) % N) * 2 + slot]
    )
    hit = owner[None, None] == wanted[:, :, None, None]
    return jnp.sum(jnp.where(hit, code[None, None], 0), axis=(2, 3)) - 1


def body(panel, owner):
    x, c, y, z = (lax.axis_index(name) for name in "xcyz")
    at = jnp.stack([z, y]).astype(jnp.int32)
    tab = tile_codes(owner, x, c, y, z)

    cuts = cut(at, panel)
    first = cuts[0]
    pieces = [shift(cuts[1 + s], "z", s + 1) for s in range(3)] + [shift(cuts[4 + s], "y", s + 1) for s in range(3)]
    rest = jnp.stack(pieces)

    firsts = [first] + [shift(first, "x", d) for d in range(1, N)]
    slabs_z = [panel] + [shift(panel, "z", s) for s in range(1, N)]
    slabs_y = [panel] + [shift(panel, "y", s) for s in range(1, N)]
    rests = [rest] + [shift(rest, "x", d) for d in range(1, N)]
    firsts += [shift(v, "c", 1) for v in firsts]
    rests += [shift(v, "c", 1) for v in rests]

    found = []
    for kind, (slabs, along, across) in enumerate(((slabs_z, "y", "z"), (slabs_y, "z", "y"))):
        sums = sum_along(along, product(kind, tab, slabs, firsts, rests))
        found += [sums[0]] + [shift(sums[s], across, s) for s in range(1, N)]
    return join(at, found)


def solution(mesh):
    grid = Mesh(mesh.devices.reshape(N, 2, N, N), ("x", "c", "y", "z"))
    return jax.shard_map(
        body,
        mesh=grid,
        in_specs=(P(("x", "c"), ("y", "z")), P()),
        out_specs=P(("x", "c"), ("y", "z"), None, None),
        check_vma=False,
    )
```

```python
import functools

import jax
import jax.numpy as jnp
from jax import lax
from jax.experimental import pallas as pl
from jax.experimental.pallas import tpu as pltpu
from jax.sharding import Mesh
from jax.sharding import PartitionSpec as P


N = 4
VMEM = pltpu.VMEM
SMEM = pltpu.SMEM
HBM = pltpu.HBM


def move(value, target):
    pairs = []
    for c in range(2):
        for y in range(N):
            for z in range(N):
                core, gather, scatter = target(c, *((y, z) if c else (z, y)))
                to = (gather, scatter) if c else (scatter, gather)
                pairs.append(((c * N + y) * N + z, (core * N + to[0] % N) * N + to[1] % N))
    return lax.ppermute(value, ("c", "y", "z"), pairs)


def along(value, step):
    return move(value, lambda c, g, r: (c, g + step, r))


def across(value, step):
    return move(value, lambda c, g, r: (c, g, r + step))


def along_other(value, step):
    return move(value, lambda c, g, r: (1 - c, g + step, r))


def over(value, axis, step):
    size = lax.axis_size(axis)
    return lax.ppermute(value, axis, [(k, (k + step) % size) for k in range(size)])


def specs(space, count):
    return [pl.BlockSpec(memory_space=space)] * count


def cut_kernel(q, at_ref, mine_ref, other_ref, *outs):
    for step in range(N):
        part = lax.rem(at_ref[1] + step, N)
        for group, ref in enumerate((mine_ref, other_ref)):
            for block in range(2):
                start = pl.multiple_of((2 * block + at_ref[0]) * N * q + part * q, q)
                row = (2 * group + block) * q
                outs[step][row : row + q, :] = ref[pl.ds(start, q), :]


def cut(at, mine, other):
    rows, inner = mine.shape
    q = rows // 16
    return pl.pallas_call(
        functools.partial(cut_kernel, q),
        out_shape=[jax.ShapeDtypeStruct((4 * q, inner), mine.dtype)] * N,
        in_specs=specs(SMEM, 1) + specs(VMEM, 2),
        out_specs=specs(VMEM, N),
        cost_estimate=pl.CostEstimate(flops=10**6, bytes_accessed=3 * rows * inner * 4, transcendentals=0),
        name="cut",
    )(at, mine, other)


def product_kernel(q, tab_ref, *refs):
    slabs, firsts, rests, outs = refs[:8], refs[8:12], refs[12:16], refs[16:24]
    a_in, b_in, a3, b3, acc, held, in_sems, out_sems = refs[24:]
    rows, inner = slabs[0].shape
    copies = []
    for s in range(N):
        now = []
        for group in range(2):
            now.append((slabs[2 * s + group], a_in.at[s, group * rows : (group + 1) * rows, :]))
        for d in range(N):
            source = firsts[d] if s == 0 else rests[d].at[s - 1]
            now.append((source, b_in.at[s, 4 * q * d : 4 * q * (d + 1), :]))
        now = [
            pltpu.make_async_copy(source, place, in_sems.at[s, k]) for k, (source, place) in enumerate(now)
        ]
        for copy in now:
            copy.start()
        copies.append(now)

    def halves(value):
        high = value.astype(jnp.bfloat16)
        return high, (value - high.astype(jnp.float32)).astype(jnp.bfloat16)

    half = rows // 2
    for s in range(N):
        for copy in copies[s]:
            copy.wait()

        def split(k, carry):
            at = pl.ds(pl.multiple_of(k * half, half), half)
            high, low = halves(a_in[s, at, :])
            a3[at, 0:inner] = high
            a3[at, inner : 2 * inner] = low
            a3[at, 2 * inner :] = high
            return carry

        lax.fori_loop(0, 4, split, 0)
        for m in range(2):
            at = slice(m * half, (m + 1) * half)
            high, low = halves(b_in[s, at, :])
            b3[at, 0:inner] = high
            b3[at, inner : 2 * inner] = high
            b3[at, 2 * inner :] = low

        def multiply(n, carry):
            right = a3[pl.ds(pl.multiple_of(n * (half // 2), half // 2), half // 2), :]
            for m in range(2):
                at = slice(m * half, (m + 1) * half)
                found = lax.dot_general(
                    b3[at, :], right, (((1,), (1,)), ((), ())), preferred_element_type=jnp.float32
                )
                acc[n, at, :] = found if s == 0 else acc[n, at, :] + found
            return carry

        lax.fori_loop(0, 8, multiply, 0)

    back = []
    order = (4, 5, 3, 6, 2, 7, 0, 1)
    for index in order:
        group = index % 2

        def place(k, carry):
            code = tab_ref[index * 8 + k]
            safe = jnp.maximum(code, 0)
            start = pl.multiple_of((safe // 2) * q, q)
            for side in range(2):
                tile = acc[group * 4 + (safe % 2) * 2 + side, pl.ds(start, q), :]
                held[index, k, :, side * (half // 2) : (side + 1) * (half // 2)] = jnp.where(code >= 0, tile, 0.0)
            return carry

        lax.fori_loop(0, 8, place, 0)
        copy = pltpu.make_async_copy(held.at[index], outs[index], out_sems.at[index])
        copy.start()
        back.append(copy)
    for copy in back:
        copy.wait()


def product(tab, slabs, firsts, rests):
    rows, inner = slabs[0].shape
    q, half = rows // 16, rows // 2
    return pl.pallas_call(
        functools.partial(product_kernel, q),
        out_shape=[jax.ShapeDtypeStruct((8, q, half), jnp.float32)] * 8,
        in_specs=specs(SMEM, 1) + specs(HBM, 16),
        out_specs=specs(HBM, 8),
        scratch_shapes=[
            VMEM((N, 2 * rows, inner), jnp.float32),
            VMEM((N, rows, inner), jnp.float32),
            VMEM((2 * rows, 3 * inner), jnp.bfloat16),
            VMEM((rows, 3 * inner), jnp.bfloat16),
            VMEM((8, rows, half // 2), jnp.float32),
            VMEM((8, 8, q, half), jnp.float32),
            pltpu.SemaphoreType.DMA((N, 6)),
            pltpu.SemaphoreType.DMA((8,)),
        ],
        compiler_params=pltpu.CompilerParams(vmem_limit_bytes=48 * 1024 * 1024),
        cost_estimate=pl.CostEstimate(
            flops=4 * rows * rows * 12 * inner, bytes_accessed=20 * rows * inner * 4, transcendentals=0
        ),
        name="product",
    )(tab, *slabs, *firsts, *rests)


def join_kernel(q, at_ref, *refs):
    pieces, out_ref, held = refs[:8], refs[8], refs[9]
    for index in range(8):
        kind = at_ref[0] if index < N else 1 - at_ref[0]
        mine = at_ref[1] if index < N else at_ref[2]
        part = lax.rem(mine + N - index % N, N)
        start = pl.multiple_of((kind * N + part) * q, q)
        for slot in range(2):
            held[slot, pl.ds(start, q), :] = pieces[index][slot]
    for slot in range(2):
        out_ref[0, slot] = held[slot].T


def join(at, pieces):
    _, q, half = pieces[0].shape
    return pl.pallas_call(
        functools.partial(join_kernel, q),
        out_shape=jax.ShapeDtypeStruct((1, 2, half, half), jnp.float32),
        in_specs=specs(SMEM, 1) + specs(VMEM, 8),
        out_specs=pl.BlockSpec(memory_space=VMEM),
        scratch_shapes=[VMEM((2, half, half), jnp.float32)],
        compiler_params=pltpu.CompilerParams(vmem_limit_bytes=32 * 1024 * 1024),
        cost_estimate=pl.CostEstimate(flops=10**6, bytes_accessed=16 * half * half, transcendentals=0),
        name="join",
    )(at, *pieces)


def tile_codes(owner, x, c, gather, scatter):
    blocks = owner.shape[0]
    i = lax.broadcasted_iota(jnp.int32, (blocks, blocks), 0)
    j = lax.broadcasted_iota(jnp.int32, (blocks, blocks), 1)
    group = j // 2
    array = ((x - group // 2 + N) % N) * 2 + jnp.where(group % 2 == c, 0, 1)
    code = jnp.where(j <= i, (array * 2 + j % 2) * 2 + i % 2 + 1, 0)
    index = jnp.arange(64, dtype=jnp.int32)
    far = (scatter + index // 16) % N
    mine = (index // 8) % 2
    near = (gather + (index // 2) % 4) % N
    wanted = jnp.where(c == 0, far * N + near, near * N + far) * 2 + index % 2
    wanted_group = 2 * x + jnp.where(mine == 0, c, 1 - c)
    hit = (owner[None] == wanted[:, None, None]) & ((i // 2)[None] == wanted_group[:, None, None])
    return jnp.sum(jnp.where(hit, code[None], 0), axis=(1, 2)) - 1


def body(panel, owner):
    x, c, y, z = (lax.axis_index(name) for name in "xcyz")
    gather, scatter = jnp.where(c == 0, z, y), jnp.where(c == 0, y, z)
    at = jnp.stack([c, gather, scatter]).astype(jnp.int32)
    tab = tile_codes(owner, x, c, gather, scatter)

    other = over(panel, "c", 1)
    first, *sends = cut(at, panel, other)
    rest = jnp.stack([along(piece, s + 1) for s, piece in enumerate(sends)])
    firsts = [first] + [over(first, "x", d) for d in range(1, N)]
    rests = [rest] + [over(rest, "x", d) for d in range(1, N)]

    up = [along(panel, 1), along(other, 1)]
    down = [along(panel, -1), along(other, -1)]
    slabs = [panel, other, *up, along(up[0], 1), along(down[1], -1), *down]

    own0, own1, near0, near1, far0, far1, last0, last1 = product(tab, slabs, firsts, rests)
    up_far, down_far = across(far0, 1), across(far1, -1)
    up_near, down_near = across(near1, 1), across(last0, -1)
    up_sum = across(near0 + up_far, 1)
    down_sum = across(last1 + down_far, -1)
    found, passed = [], []
    for s in range(N):
        part = slice(2 * s, 2 * s + 2)
        mine = own0[part] + up_sum[part] + down_near[part]
        theirs = own1[part] + down_sum[part] + up_near[part]
        found.append(mine if s == 0 else along(mine, s))
        passed.append(along_other(theirs, s))
    return join(at, found + passed)


def solution(mesh):
    grid = Mesh(mesh.devices.reshape(N, 2, N, N), ("x", "c", "y", "z"))
    return jax.shard_map(
        body,
        mesh=grid,
        in_specs=(P(("x", "c"), ("y", "z")), P()),
        out_specs=P(("x", "c"), ("y", "z"), None, None),
        check_vma=False,
    )
```

```python
import functools

import jax
import jax.numpy as jnp
from jax import lax
from jax.experimental import pallas as pl
from jax.experimental.pallas import tpu as pltpu
from jax.sharding import Mesh
from jax.sharding import PartitionSpec as P


N = 4
VMEM = pltpu.VMEM
SMEM = pltpu.SMEM
HBM = pltpu.HBM


def move(value, target):
    pairs = []
    for c in range(2):
        for y in range(N):
            for z in range(N):
                core, gather, scatter = target(c, *((y, z) if c else (z, y)))
                to = (gather, scatter) if c else (scatter, gather)
                pairs.append(((c * N + y) * N + z, (core * N + to[0] % N) * N + to[1] % N))
    return lax.ppermute(value, ("c", "y", "z"), pairs)


def along(value, step):
    return move(value, lambda c, g, r: (c, g + step, r))


def across(value, step):
    return move(value, lambda c, g, r: (c, g, r + step))


def along_other(value, step):
    return move(value, lambda c, g, r: (1 - c, g + step, r))


def over(value, axis, step):
    size = lax.axis_size(axis)
    pairs = [(k, (k + step) % size) for k in range(size) if axis == "c" or k + step < size]
    return lax.ppermute(value, axis, pairs)


def specs(space, count):
    return [pl.BlockSpec(memory_space=space)] * count


def cut_kernel(q, at_ref, mine_ref, other_ref, *outs):
    for step in range(N):
        part = lax.rem(at_ref[1] + step, N)
        for group, ref in enumerate((mine_ref, other_ref)):
            for block in range(2):
                start = pl.multiple_of((2 * block + at_ref[0]) * N * q + part * q, q)
                row = (2 * group + block) * q
                outs[step][row : row + q, :] = ref[pl.ds(start, q), :]


def cut(at, mine, other):
    rows, inner = mine.shape
    q = rows // 16
    return pl.pallas_call(
        functools.partial(cut_kernel, q),
        out_shape=[jax.ShapeDtypeStruct((4 * q, inner), mine.dtype)] * N,
        in_specs=specs(SMEM, 1) + specs(VMEM, 2),
        out_specs=specs(VMEM, N),
        cost_estimate=pl.CostEstimate(flops=10**6, bytes_accessed=3 * rows * inner * 4, transcendentals=0),
        name="cut",
    )(at, mine, other)


def product_kernel(q, slabs, first, last, tab_ref, *refs):
    a_refs, refs = refs[: 2 * slabs], refs[2 * slabs :]
    b_refs, refs = refs[:N], refs[N:]
    total_ref, refs = (None, refs) if first else (refs[0], refs[1:])
    outs, refs = refs[: 8 if last else 1], refs[8 if last else 1 :]
    a_in, b_in, a3, b3, acc, in_sems, total_sem, out_sems, *held = refs
    rows, inner = a_refs[0].shape
    half, side = rows // 2, rows // 4
    copies = []
    for s in range(slabs):
        now = [(a_refs[2 * s + group], a_in.at[s, group * rows : (group + 1) * rows, :]) for group in range(2)]
        for d in range(N):
            now.append((b_refs[d].at[s], b_in.at[s, 4 * q * d : 4 * q * (d + 1), :]))
        now = [pltpu.make_async_copy(source, place, in_sems.at[s, k]) for k, (source, place) in enumerate(now)]
        for copy in now:
            copy.start()
        copies.append(now)
        if s == 0 and not first:
            total = pltpu.make_async_copy(total_ref, acc, total_sem.at[0])
            total.start()

    def halves(value):
        high = value.astype(jnp.bfloat16)
        return high, (value - high.astype(jnp.float32)).astype(jnp.bfloat16)

    def write(place, source, index):
        copy = pltpu.make_async_copy(source, place, out_sems.at[index])
        copy.start()
        return copy

    back = []
    for s in range(slabs):
        for copy in copies[s]:
            copy.wait()

        def split(k, carry):
            at = pl.ds(pl.multiple_of(k * half, half), half)
            high, low = halves(a_in[s, at, :])
            a3[at, 0:inner] = high
            a3[at, inner : 2 * inner] = low
            a3[at, 2 * inner :] = high
            return carry

        lax.fori_loop(0, 4, split, 0)
        for m in range(2):
            at = slice(m * half, (m + 1) * half)
            high, low = halves(b_in[s, at, :])
            b3[at, 0:inner] = high
            b3[at, inner : 2 * inner] = high
            b3[at, 2 * inner :] = low
        if s == 0 and not first:
            total.wait()

        def multiply(pair, carry):
            for part in range(2):
                n = 2 * pair + part
                right = a3[pl.ds(pl.multiple_of(n * side, side), side), :]
                for m in range(2):
                    at = slice(m * half, (m + 1) * half)
                    found = lax.dot_general(
                        b3[at, :], right, (((1,), (1,)), ((), ())), preferred_element_type=jnp.float32
                    )
                    acc[n, at, :] = found if first and s == 0 else acc[n, at, :] + found
            return carry

        if s < slabs - 1:
            lax.fori_loop(0, 4, multiply, 0)

    for group in range(2):
        lax.fori_loop(2 * group, 2 * group + 2, multiply, 0)
        if not last:
            part = slice(4 * group, 4 * group + 4)
            back.append(write(outs[0].at[part], acc.at[part], group))
            continue
        for chunk in (2, 1, 3, 0):
            index = 2 * chunk + group

            def place(k, carry):
                code = tab_ref[index * 8 + k]
                safe = jnp.maximum(code, 0)
                start = pl.multiple_of((safe // 2) * q, q)
                for b in range(2):
                    tile = acc[group * 4 + (safe % 2) * 2 + b, pl.ds(start, q), :]
                    held[0][index, k, :, b * side : (b + 1) * side] = jnp.where(code >= 0, tile, 0.0)
                return carry

            lax.fori_loop(0, 8, place, 0)
            back.append(write(outs[index], held[0].at[index], index))
    for copy in back:
        copy.wait()


def product(tab, slabs, slices, total, last):
    rows, inner = slabs[0].shape
    q, half, count = rows // 16, rows // 2, len(slabs) // 2
    first = total is None
    if last:
        out_shape = [jax.ShapeDtypeStruct((8, q, half), jnp.float32)] * 8
    else:
        out_shape = [jax.ShapeDtypeStruct((8, rows, half // 2), jnp.float32)]
    totals = [] if first else [total]
    return pl.pallas_call(
        functools.partial(product_kernel, q, count, first, last),
        out_shape=out_shape,
        in_specs=specs(SMEM, 1) + specs(HBM, 2 * count + N + len(totals)),
        out_specs=specs(HBM, len(out_shape)),
        scratch_shapes=[
            VMEM((count, 2 * rows, inner), jnp.float32),
            VMEM((count, rows, inner), jnp.float32),
            VMEM((2 * rows, 3 * inner), jnp.bfloat16),
            VMEM((rows, 3 * inner), jnp.bfloat16),
            VMEM((8, rows, half // 2), jnp.float32),
            pltpu.SemaphoreType.DMA((count, 6)),
            pltpu.SemaphoreType.DMA((1,)),
            pltpu.SemaphoreType.DMA((8,)),
        ]
        + ([VMEM((8, 8, q, half), jnp.float32)] if last else []),
        compiler_params=pltpu.CompilerParams(vmem_limit_bytes=40 * 1024 * 1024),
        cost_estimate=pl.CostEstimate(
            flops=4 * rows * rows * 3 * inner * count, bytes_accessed=12 * rows * inner * 4, transcendentals=0
        ),
    )(tab, *slabs, *slices, *totals)


def join_kernel(q, at_ref, *refs):
    pieces, out_ref, held = refs[:8], refs[8], refs[9]
    for index in range(8):
        kind = at_ref[0] if index < N else 1 - at_ref[0]
        mine = at_ref[1] if index < N else at_ref[2]
        part = lax.rem(mine + N - index % N, N)
        start = pl.multiple_of((kind * N + part) * q, q)
        for slot in range(2):
            held[slot, pl.ds(start, q), :] = pieces[index][slot]
    for slot in range(2):
        out_ref[0, slot] = held[slot].T


def join(at, pieces):
    _, q, half = pieces[0].shape
    return pl.pallas_call(
        functools.partial(join_kernel, q),
        out_shape=jax.ShapeDtypeStruct((1, 2, half, half), jnp.float32),
        in_specs=specs(SMEM, 1) + specs(VMEM, 8),
        out_specs=pl.BlockSpec(memory_space=VMEM),
        scratch_shapes=[VMEM((2, half, half), jnp.float32)],
        compiler_params=pltpu.CompilerParams(vmem_limit_bytes=32 * 1024 * 1024),
        cost_estimate=pl.CostEstimate(flops=10**6, bytes_accessed=16 * half * half, transcendentals=0),
        name="join",
    )(at, *pieces)


def tile_codes(owner, x, c, gather, scatter):
    blocks = owner.shape[0]
    i = lax.broadcasted_iota(jnp.int32, (blocks, blocks), 0)
    j = lax.broadcasted_iota(jnp.int32, (blocks, blocks), 1)
    group = j // 2
    array = ((x - group // 2 + N) % N) * 2 + jnp.where(group % 2 == c, 0, 1)
    code = jnp.where(j <= i, (array * 2 + j % 2) * 2 + i % 2 + 1, 0)
    index = jnp.arange(64, dtype=jnp.int32)
    far = (scatter + index // 16) % N
    mine = (index // 8) % 2
    near = (gather + (index // 2) % 4) % N
    wanted = jnp.where(c == 0, far * N + near, near * N + far) * 2 + index % 2
    wanted_group = 2 * x + jnp.where(mine == 0, c, 1 - c)
    hit = (owner[None] == wanted[:, None, None]) & ((i // 2)[None] == wanted_group[:, None, None])
    return jnp.sum(jnp.where(hit, code[None], 0), axis=(1, 2)) - 1


def update(panel, owner):
    x, c, y, z = (lax.axis_index(name) for name in "xcyz")
    gather, scatter = jnp.where(c == 0, z, y), jnp.where(c == 0, y, z)
    at = jnp.stack([c, gather, scatter]).astype(jnp.int32)
    tab = tile_codes(owner, x, c, gather, scatter)

    other = over(panel, "c", 1)
    first, *sends = cut(at, panel, other)
    small = [along(sends[s - 1], s) for s in range(1, N)]
    slices = []
    for piece in (first[None], jnp.stack([small[0], small[2]]), small[1][None]):
        slices.append([piece] + [over(piece, "x", d) for d in range(1, N)])

    up = [along(panel, 1), along(other, 1)]
    down = [along(panel, -1), along(other, -1)]
    beyond = [along(up[0], 1), along(down[1], -1)]

    (total,) = product(tab, [panel, other], slices[0], None, False)
    (total,) = product(tab, up + down, slices[1], total, False)
    own0, own1, near0, near1, far0, far1, last0, last1 = product(tab, beyond, slices[2], total, True)

    up_far, down_far = across(far0, 1), across(far1, -1)
    up_near, down_near = across(near1, 1), across(last0, -1)
    up_sum = across(near0 + up_far, 1)
    down_sum = across(last1 + down_far, -1)
    found, passed = [], []
    for s in range(N):
        part = slice(2 * s, 2 * s + 2)
        mine = own0[part] + up_sum[part] + down_near[part]
        theirs = own1[part] + down_sum[part] + up_near[part]
        found.append(mine if s == 0 else along(mine, s))
        passed.append(along_other(theirs, s))
    return join(at, found + passed)


def solution(mesh):
    grid = Mesh(mesh.devices.reshape(N, 2, N, N), ("x", "c", "y", "z"))
    return jax.shard_map(
        update,
        mesh=grid,
        in_specs=(P(("x", "c"), ("y", "z")), P()),
        out_specs=P(("x", "c"), ("y", "z"), None, None),
        check_vma=False,
    )
```

```python
import functools

import jax
import jax.numpy as jnp
from jax import lax
from jax.experimental import pallas as pl
from jax.experimental.pallas import tpu as pltpu
from jax.sharding import Mesh
from jax.sharding import PartitionSpec as P


N = 4
VMEM = pltpu.VMEM
SMEM = pltpu.SMEM
HBM = pltpu.HBM
GRANT = 60 * 1024 * 1024


def move(value, target):
    pairs = []
    for c in range(2):
        for y in range(N):
            for z in range(N):
                core, gather, scatter = target(c, *((y, z) if c else (z, y)))
                to = (gather, scatter) if c else (scatter, gather)
                pairs.append(((c * N + y) * N + z, (core * N + to[0] % N) * N + to[1] % N))
    return lax.ppermute(value, ("c", "y", "z"), pairs)


def along(value, step):
    return move(value, lambda c, g, r: (c, g + step, r))


def across(value, step):
    return move(value, lambda c, g, r: (c, g, r + step))


def along_other(value, step):
    return move(value, lambda c, g, r: (1 - c, g + step, r))


def swap(value):
    return lax.ppermute(value, "c", [(0, 1), (1, 0)])


def hop(value, pairs):
    return lax.ppermute(value, "x", pairs)


def specs(space, count):
    return [pl.BlockSpec(memory_space=space)] * count


def cut_kernel(q, at_ref, mine_ref, other_ref, *outs):
    for step in range(N):
        part = lax.rem(at_ref[1] + step, N)
        for group, ref in enumerate((mine_ref, other_ref)):
            for block in range(2):
                start = pl.multiple_of((2 * block + at_ref[0]) * N * q + part * q, q)
                row = (2 * group + block) * q
                outs[step][row : row + q, :] = ref[pl.ds(start, q), :]


def cut(at, mine, other):
    rows, inner = mine.shape
    q = rows // 16
    return pl.pallas_call(
        functools.partial(cut_kernel, q),
        out_shape=[jax.ShapeDtypeStruct((4 * q, inner), mine.dtype)] * N,
        in_specs=specs(SMEM, 1) + specs(VMEM, 2),
        out_specs=specs(VMEM, N),
        cost_estimate=pl.CostEstimate(flops=10**6, bytes_accessed=3 * rows * inner * 4, transcendentals=0),
        name="cut",
    )(at, mine, other)


def split_kernel(*refs):
    for source, place in zip(refs[:2], refs[2:]):
        value = source[...]
        inner = value.shape[1]
        high = value.astype(jnp.bfloat16)
        place[:, :inner] = high
        place[:, inner:] = (value - high.astype(jnp.float32)).astype(jnp.bfloat16)


def split(pair):
    rows, inner = pair[0].shape
    block = rows // 4
    return pl.pallas_call(
        split_kernel,
        grid=(4,),
        out_shape=[jax.ShapeDtypeStruct((rows, 2 * inner), jnp.bfloat16)] * 2,
        in_specs=[pl.BlockSpec((block, inner), lambda i: (i, 0))] * 2,
        out_specs=[pl.BlockSpec((block, 2 * inner), lambda i: (i, 0))] * 2,
        cost_estimate=pl.CostEstimate(flops=10**6, bytes_accessed=16 * rows * inner, transcendentals=0),
        compiler_params=pltpu.CompilerParams(vmem_limit_bytes=GRANT),
    )(*pair)


def product_kernel(q, work, totals, last, tab_ref, *refs):
    count = len(work)
    a_refs, refs = refs[: 2 * count], refs[2 * count :]
    b_refs = []
    for places in work:
        b_refs.append(refs[: len(places)])
        refs = refs[len(places) :]
    total_refs, refs = refs[: len(totals)], refs[len(totals) :]
    outs, refs = refs[: 8 if last else 1], refs[8 if last else 1 :]
    a_in, b_in, b2, acc, a_sems, b_sems, total_sems, out_sems, *held = refs
    rows, inner = a_refs[0].shape[0], a_refs[0].shape[1] // 2
    side, wide = rows // 4, 4 * q

    def begin(source, place, sem):
        copy = pltpu.make_async_copy(source, place, sem)
        copy.start()
        return copy

    loads, waits = [], []
    for k, places in enumerate(work):
        now = [
            begin(
                b_refs[k][m].at[row : row + wide, :], b_in.at[k, wide * place : wide * (place + 1), :], b_sems.at[k, m]
            )
            for m, (place, row) in enumerate(places)
        ]
        for group in range(2):
            now.append(
                begin(a_refs[2 * k + group], a_in.at[k, group * rows : (group + 1) * rows, :], a_sems.at[k, group])
            )
        loads.append(now)
        if k == 0:
            for m, (ref, (low, high)) in enumerate(zip(total_refs, totals)):
                part = (slice(None), slice(wide * low, wide * high), slice(None))
                waits.append(begin(ref.at[part], acc.at[part], total_sems.at[m]))

    back = []
    fresh = not totals
    for k, places in enumerate(work):
        for copy in loads[k]:
            copy.wait()
        first, stop = places[0][0], places[-1][0] + 1
        pieces = [(m, min(m + 2, stop)) for m in range(first, stop, 2)]
        for low, high in pieces:
            at = slice(wide * low, wide * high)
            value = b_in[k, at, :]
            upper = value.astype(jnp.bfloat16)
            b2[at, :inner] = upper
            b2[at, inner:] = (value - upper.astype(jnp.float32)).astype(jnp.bfloat16)
        if k == 0:
            for copy in waits:
                copy.wait()

        def multiply(pair, carry):
            for part in range(2):
                n = 2 * pair + part
                right = a_in[k, pl.ds(pl.multiple_of(n * side, side), side), :]
                right = jnp.concatenate([right, right[:, :inner]], axis=1)
                for low, high in pieces:
                    at = slice(wide * low, wide * high)
                    left = jnp.concatenate([b2[at, :inner], b2[at, :]], axis=1)
                    found = lax.dot_general(
                        left, right, (((1,), (1,)), ((), ())), preferred_element_type=jnp.float32
                    )
                    acc[n, at, :] = found if fresh and k == 0 else acc[n, at, :] + found
            return carry

        if k < count - 1:
            lax.fori_loop(0, 4, multiply, 0)

    for group in range(2):
        lax.fori_loop(2 * group, 2 * group + 2, multiply, 0)
        if not last:
            part = (slice(4 * group, 4 * group + 4), slice(wide * work[0][0][0], wide * (work[0][-1][0] + 1)), slice(None))
            back.append(begin(acc.at[part], outs[0].at[part], out_sems.at[group]))
            continue
        for chunk in (2, 1, 3, 0):
            index = 2 * chunk + group

            def place(k, carry):
                code = tab_ref[index * 8 + k]
                safe = jnp.maximum(code, 0)
                start = pl.multiple_of((safe // 2) * q, q)
                for b in range(2):
                    tile = acc[group * 4 + (safe % 2) * 2 + b, pl.ds(start, q), :]
                    held[0][index, k, :, b * side : (b + 1) * side] = jnp.where(code >= 0, tile, 0.0)
                return carry

            lax.fori_loop(0, 8, place, 0)
            back.append(begin(held[0].at[index], outs[index], out_sems.at[index]))
    for copy in back:
        copy.wait()


def product(tab, work, totals, last):
    rows, inner = work[0][0][0].shape[0], work[0][0][0].shape[1] // 2
    q, half, count = rows // 16, rows // 2, len(work)
    if last:
        out_shape = [jax.ShapeDtypeStruct((8, q, half), jnp.float32)] * 8
    else:
        out_shape = [jax.ShapeDtypeStruct((8, rows, half // 2), jnp.float32)]
    a_args = [part for parts, _ in work for part in parts]
    b_args = [piece for _, slices in work for piece, _ in slices.values()]
    places = tuple(tuple((place, row) for place, (_, row) in slices.items()) for _, slices in work)
    return pl.pallas_call(
        functools.partial(product_kernel, q, places, tuple(span for _, span in totals), last),
        out_shape=out_shape,
        in_specs=specs(SMEM, 1) + specs(HBM, len(a_args) + len(b_args) + len(totals)),
        out_specs=specs(HBM, len(out_shape)),
        scratch_shapes=[
            VMEM((count, 2 * rows, 2 * inner), jnp.bfloat16),
            VMEM((count, rows, inner), jnp.float32),
            VMEM((rows, 2 * inner), jnp.bfloat16),
            VMEM((8, rows, half // 2), jnp.float32),
            pltpu.SemaphoreType.DMA((count, 2)),
            pltpu.SemaphoreType.DMA((count, N)),
            pltpu.SemaphoreType.DMA((2,)),
            pltpu.SemaphoreType.DMA((8,)),
        ]
        + ([VMEM((8, 8, q, half), jnp.float32)] if last else []),
        compiler_params=pltpu.CompilerParams(vmem_limit_bytes=GRANT),
        cost_estimate=pl.CostEstimate(
            flops=4 * rows * rows * 3 * inner * count, bytes_accessed=12 * rows * inner * 4, transcendentals=0
        ),
    )(tab, *a_args, *b_args, *(total for total, _ in totals))


def join_kernel(q, at_ref, *refs):
    pieces, out_ref, held = refs[:8], refs[8], refs[9]
    for index in range(8):
        kind = at_ref[0] if index < N else 1 - at_ref[0]
        mine = at_ref[1] if index < N else at_ref[2]
        part = lax.rem(mine + N - index % N, N)
        start = pl.multiple_of((kind * N + part) * q, q)
        for slot in range(2):
            held[slot, pl.ds(start, q), :] = pieces[index][slot]
    for slot in range(2):
        out_ref[0, slot] = held[slot].T


def join(at, pieces):
    _, q, half = pieces[0].shape
    return pl.pallas_call(
        functools.partial(join_kernel, q),
        out_shape=jax.ShapeDtypeStruct((1, 2, half, half), jnp.float32),
        in_specs=specs(SMEM, 1) + specs(VMEM, 8),
        out_specs=pl.BlockSpec(memory_space=VMEM),
        scratch_shapes=[VMEM((2, half, half), jnp.float32)],
        compiler_params=pltpu.CompilerParams(vmem_limit_bytes=32 * 1024 * 1024),
        cost_estimate=pl.CostEstimate(flops=10**6, bytes_accessed=16 * half * half, transcendentals=0),
        name="join",
    )(at, *pieces)


def tile_codes(owner, x, c, gather, scatter):
    blocks = owner.shape[0]
    i = lax.broadcasted_iota(jnp.int32, (blocks, blocks), 0)
    j = lax.broadcasted_iota(jnp.int32, (blocks, blocks), 1)
    group = j // 2
    behind = (x - group // 2 + N) % N
    array = jnp.where(behind < 2, behind, 5 - behind) * 2 + jnp.where(group % 2 == c, 0, 1)
    code = jnp.where(j <= i, (array * 2 + j % 2) * 2 + i % 2 + 1, 0)
    index = jnp.arange(64, dtype=jnp.int32)
    far = (scatter + index // 16) % N
    mine = (index // 8) % 2
    near = (gather + (index // 2) % 4) % N
    wanted = jnp.where(c == 0, far * N + near, near * N + far) * 2 + index % 2
    wanted_group = 2 * x + jnp.where(mine == 0, c, 1 - c)
    hit = (owner[None] == wanted[:, None, None]) & ((i // 2)[None] == wanted_group[:, None, None])
    return jnp.sum(jnp.where(hit, code[None], 0), axis=(1, 2)) - 1


def update(panel, owner):
    x, c, y, z = (lax.axis_index(name) for name in "xcyz")
    gather, scatter = jnp.where(c == 0, z, y), jnp.where(c == 0, y, z)
    at = jnp.stack([c, gather, scatter]).astype(jnp.int32)
    tab = tile_codes(owner, x, c, gather, scatter)

    other = swap(panel)
    up, down = [along(panel, 1)], [along(panel, -1)]
    first, *sends = cut(at, panel, other)
    small = [along(sends[s - 1], s) for s in range(1, N)]
    up.append(along(other, 1))
    down.append(along(other, -1))
    beyond = [along(up[0], 1), along(down[1], -1)]

    onward, wrap = [(0, 1), (1, 2), (2, 3)], [(0, 3)]
    both = jnp.concatenate([small[0], small[2]])
    a1, a3 = hop(first, onward), hop(first, wrap)
    b1, b3 = hop(both, onward), hop(both, wrap + [(1, 0)])
    c1, c3 = hop(small[1], onward), hop(small[1], wrap)
    a2, c2 = hop(a1, onward[1:]), hop(c1, onward[1:])
    b2 = hop(b3, wrap + [(3, 2)])

    own_parts = split([panel, other])
    up_parts, down_parts = split(up), split(down)
    far_parts = split(beyond)
    wide = first.shape[0]
    low, high = [(v, 0) for v in (both, b1, b3, b2)], [(v, wide) for v in (both, b1, b3, b2)]
    zero, far = [(v, 0) for v in (first, a1, a3, a2)], [(v, 0) for v in (small[1], c1, c3, c2)]
    three, four = range(3), range(4)
    (base,) = product(tab, [(own_parts, dict(zip(four, zero)))], [], False)
    (total,) = product(
        tab, [(up_parts, dict(zip(three, low))), (down_parts, dict(zip(three, high)))], [(base, (0, 3))], False
    )
    outs = product(
        tab,
        [(up_parts, {3: low[3]}), (down_parts, {3: high[3]}), (far_parts, dict(zip(four, far)))],
        [(total, (0, 3)), (base, (3, 4))],
        True,
    )
    own0, own1, near0, near1, far0, far1, last0, last1 = outs


    up_far, down_far = across(far0, 1), across(far1, -1)
    up_near, down_near = across(near1, 1), across(last0, -1)
    up_sum = across(near0 + up_far, 1)
    down_sum = across(last1 + down_far, -1)
    found, passed = [], []
    for s in range(N):
        part = slice(2 * s, 2 * s + 2)
        mine = own0[part] + up_sum[part] + down_near[part]
        theirs = own1[part] + down_sum[part] + up_near[part]
        found.append(mine if s == 0 else along(mine, s))
        passed.append(along_other(theirs, s))
    return join(at, found + passed)


def solution(mesh):
    grid = Mesh(mesh.devices.reshape(N, 2, N, N), ("x", "c", "y", "z"))
    return jax.shard_map(
        update,
        mesh=grid,
        in_specs=(P(("x", "c"), ("y", "z")), P()),
        out_specs=P(("x", "c"), ("y", "z"), None, None),
        check_vma=False,
    )
```

```python
import functools

import jax
import jax.numpy as jnp
from jax import lax
from jax.experimental import pallas as pl
from jax.experimental.pallas import tpu as pltpu
from jax.sharding import Mesh
from jax.sharding import PartitionSpec as P


N = 4
VMEM = pltpu.VMEM
SMEM = pltpu.SMEM
GRANT = 16 * 1024 * 1024


def move(value, target):
    pairs = []
    for c in range(2):
        for y in range(N):
            for z in range(N):
                core, gather, scatter = target(c, *((y, z) if c else (z, y)))
                to = (gather, scatter) if c else (scatter, gather)
                pairs.append(((c * N + y) * N + z, (core * N + to[0] % N) * N + to[1] % N))
    return lax.ppermute(value, ("c", "y", "z"), pairs)


def along(value, step):
    return move(value, lambda c, g, r: (c, g + step, r))


def across(value, step):
    return move(value, lambda c, g, r: (c, g, r + step))


def along_other(value, step):
    return move(value, lambda c, g, r: (1 - c, g + step, r))


def swap(value):
    return lax.ppermute(value, "c", [(0, 1), (1, 0)])


def hop(value, pairs):
    return lax.ppermute(value, "x", pairs)


def specs(space, count):
    return [pl.BlockSpec(memory_space=space)] * count


def cut_kernel(q, at_ref, mine_ref, other_ref, *outs):
    for step in range(N):
        part = lax.rem(at_ref[1] + step, N)
        for group, ref in enumerate((mine_ref, other_ref)):
            for block in range(2):
                start = pl.multiple_of((2 * block + at_ref[0]) * N * q + part * q, q)
                row = (2 * group + block) * q
                outs[step][row : row + q, :] = ref[pl.ds(start, q), :]


def cut(at, mine, other):
    rows, inner = mine.shape
    q = rows // 16
    return pl.pallas_call(
        functools.partial(cut_kernel, q),
        out_shape=[jax.ShapeDtypeStruct((4 * q, inner), mine.dtype)] * N,
        in_specs=specs(SMEM, 1) + specs(VMEM, 2),
        out_specs=specs(VMEM, N),
        compiler_params=pltpu.CompilerParams(vmem_limit_bytes=GRANT),
        cost_estimate=pl.CostEstimate(flops=10**6, bytes_accessed=3 * rows * inner * 4, transcendentals=0),
        name="cut",
    )(at, mine, other)


def product_kernel(q, work, carried, last, tab_ref, *refs):
    slabs = []
    for raw, places in work:
        a_refs, refs = refs[: 2 if raw else 1], refs[2 if raw else 1 :]
        slabs.append((raw, a_refs, list(zip(places, refs))))
        refs = refs[len(places) :]
    total_ref, refs = (refs[0], refs[1:]) if carried else (None, refs)
    raws = sum(raw for raw, _ in work)
    if last:
        outs, (acc, b_parts, *a_parts) = refs[:8], refs[8:]
    else:
        acc, a_parts, b_parts = refs[0], list(refs[1 : 1 + raws]), refs[-1]
    wide, side = 4 * q, 4 * q

    def halves(value, place, at):
        inner = value.shape[1]
        high = value.astype(jnp.bfloat16)
        place[at, :inner] = high
        place[at, inner:] = (value - high.astype(jnp.float32)).astype(jnp.bfloat16)

    terms = {}
    used = 0
    for raw, a_refs, pieces in slabs:
        if raw:
            parts = a_parts.pop(0)
            rows = a_refs[0].shape[0]
            for group in range(2):
                halves(a_refs[group][...], parts, slice(group * rows, (group + 1) * rows))
        else:
            parts = a_refs[0]
        for (place, row), ref in pieces:
            at = slice(wide * used, wide * (used + 1))
            halves(ref[row : row + wide, :], b_parts, at)
            terms.setdefault(place, []).append((parts, at))
            used += 1

    for n in range(8):
        columns = slice(n * side, (n + 1) * side)
        for place, pairs in terms.items():
            found = None
            for parts, at in pairs:
                inner = parts.shape[1] // 2
                for left, right in ((0, 0), (0, 1), (1, 0)):
                    one = lax.dot_general(
                        b_parts[at, left * inner : (left + 1) * inner],
                        parts[columns, right * inner : (right + 1) * inner],
                        (((1,), (1,)), ((), ())),
                        preferred_element_type=jnp.float32,
                    )
                    found = one if found is None else found + one
            rows = slice(wide * place, wide * (place + 1))
            if carried and place < 3:
                found = total_ref[n, rows, :] + found
            acc[n, rows, :] = found

    if last:
        for index in range(8):

            def place(k, carry, index=index):
                code = tab_ref[index * 8 + k]
                safe = jnp.maximum(code, 0)
                start = pl.multiple_of((safe // 2) * q, q)
                for b in range(2):
                    tile = acc[(index % 2) * 4 + (safe % 2) * 2 + b, pl.ds(start, q), :]
                    outs[index][k, :, b * side : (b + 1) * side] = jnp.where(code >= 0, tile, 0.0)
                return carry

            lax.fori_loop(0, 8, place, 0, unroll=4)


def product(tab, work, total, last):
    args, form, raws, used = [tab], [], 0, 0
    for rows, slices in work:
        args += list(rows) + [piece for piece, _ in slices.values()]
        raw = len(rows) == 2
        raws, used = raws + raw, used + len(slices)
        form.append((raw, tuple((place, row) for place, (_, row) in slices.items())))
    inner = work[0][1][0][0].shape[1] if 0 in work[0][1] else work[0][1][3][0].shape[1]
    wide = inner
    q, rows = wide // 4, 4 * wide
    if total is not None:
        args.append(total)
    parts = jax.ShapeDtypeStruct((2 * rows, 2 * inner), jnp.bfloat16)
    b_scratch = VMEM((wide * used, 2 * inner), jnp.bfloat16)
    if last:
        out_shape = [jax.ShapeDtypeStruct((8, q, rows // 2), jnp.float32)] * 8
        scratch = [VMEM((8, rows, wide), jnp.float32), b_scratch] + [VMEM(parts.shape, parts.dtype)] * raws
    else:
        out_shape = [jax.ShapeDtypeStruct((8, 3 * wide, wide), jnp.float32)] + [parts] * raws
        scratch = [b_scratch]
    return pl.pallas_call(
        functools.partial(product_kernel, q, form, total is not None, last),
        out_shape=out_shape,
        in_specs=specs(SMEM, 1) + specs(VMEM, len(args) - 1),
        out_specs=specs(VMEM, len(out_shape)),
        scratch_shapes=scratch,
        input_output_aliases={} if last or total is None else {len(args) - 1: 0},
        compiler_params=pltpu.CompilerParams(vmem_limit_bytes=GRANT),
        cost_estimate=pl.CostEstimate(
            flops=24 * rows * rows * inner, bytes_accessed=12 * rows * inner * 4, transcendentals=0
        ),
    )(*args)


def join_kernel(q, at_ref, *refs):
    pieces, out_ref, held = refs[:8], refs[8], refs[9]
    for index in range(8):
        kind = at_ref[0] if index < N else 1 - at_ref[0]
        mine = at_ref[1] if index < N else at_ref[2]
        part = lax.rem(mine + N - index % N, N)
        start = pl.multiple_of((kind * N + part) * q, q)
        for slot in range(2):
            held[slot, pl.ds(start, q), :] = pieces[index][slot]
    for slot in range(2):
        out_ref[0, slot] = held[slot].T


def join(at, pieces):
    _, q, half = pieces[0].shape
    return pl.pallas_call(
        functools.partial(join_kernel, q),
        out_shape=jax.ShapeDtypeStruct((1, 2, half, half), jnp.float32),
        in_specs=specs(SMEM, 1) + specs(VMEM, 8),
        out_specs=pl.BlockSpec(memory_space=VMEM),
        scratch_shapes=[VMEM((2, half, half), jnp.float32)],
        compiler_params=pltpu.CompilerParams(vmem_limit_bytes=GRANT),
        cost_estimate=pl.CostEstimate(flops=10**6, bytes_accessed=16 * half * half, transcendentals=0),
        name="join",
    )(at, *pieces)


def tile_codes(owner, x, c, gather, scatter):
    blocks = owner.shape[0]
    i = lax.broadcasted_iota(jnp.int32, (blocks, blocks), 0)
    j = lax.broadcasted_iota(jnp.int32, (blocks, blocks), 1)
    group = j // 2
    behind = (x - group // 2 + N) % N
    array = jnp.where(behind < 2, behind, 5 - behind) * 2 + jnp.where(group % 2 == c, 0, 1)
    code = jnp.where(j <= i, (array * 2 + j % 2) * 2 + i % 2 + 1, 0)
    index = jnp.arange(64, dtype=jnp.int32)
    far = (scatter + index // 16) % N
    mine = (index // 8) % 2
    near = (gather + (index // 2) % 4) % N
    wanted = jnp.where(c == 0, far * N + near, near * N + far) * 2 + index % 2
    wanted_group = 2 * x + jnp.where(mine == 0, c, 1 - c)
    hit = (owner[None] == wanted[:, None, None]) & ((i // 2)[None] == wanted_group[:, None, None])
    return jnp.sum(jnp.where(hit, code[None], 0), axis=(1, 2)) - 1


def update(panel, owner):
    x, c, y, z = (lax.axis_index(name) for name in "xcyz")
    gather, scatter = jnp.where(c == 0, z, y), jnp.where(c == 0, y, z)
    at = jnp.stack([c, gather, scatter]).astype(jnp.int32)
    tab = tile_codes(owner, x, c, gather, scatter)

    other = swap(panel)
    up, down = [along(panel, 1)], [along(panel, -1)]
    first, *sends = cut(at, panel, other)
    small = [along(sends[s - 1], s) for s in range(1, N)]
    up.append(along(other, 1))
    down.append(along(other, -1))
    beyond = [along(up[0], 1), along(down[1], -1)]

    onward, wrap = [(0, 1), (1, 2), (2, 3)], [(0, 3)]
    both = jnp.concatenate([small[0], small[2]])
    a1, a3 = hop(first, onward), hop(first, wrap)
    b1, b3 = hop(both, onward), hop(both, wrap + [(1, 0)])
    c1, c3 = hop(small[1], onward), hop(small[1], wrap)
    a2, c2 = hop(a1, onward[1:]), hop(c1, onward[1:])
    b2 = hop(b3, wrap + [(3, 2)])

    wide = first.shape[0]
    low, high = [(v, 0) for v in (both, b1, b3, b2)], [(v, wide) for v in (both, b1, b3, b2)]
    zero, far = [(v, 0) for v in (first, a1, a3, a2)], [(v, 0) for v in (small[1], c1, c3, c2)]
    three, four = range(3), range(4)
    total, own_parts = product(tab, [((panel, other), dict(zip(three, zero)))], None, False)
    total, up_parts, down_parts = product(
        tab, [(up, dict(zip(three, low))), (down, dict(zip(three, high)))], total, False
    )
    outs = product(
        tab,
        [
            (beyond, dict(zip(four, far))),
            ((own_parts,), {3: zero[3]}),
            ((up_parts,), {3: low[3]}),
            ((down_parts,), {3: high[3]}),
        ],
        total,
        True,
    )
    own0, own1, near0, near1, far0, far1, last0, last1 = outs


    up_far, down_far = across(far0, 1), across(far1, -1)
    up_near, down_near = across(near1, 1), across(last0, -1)
    up_sum = across(near0 + up_far, 1)
    down_sum = across(last1 + down_far, -1)
    found, passed = [], []
    for s in range(N):
        part = slice(2 * s, 2 * s + 2)
        mine = own0[part] + up_sum[part] + down_near[part]
        theirs = own1[part] + down_sum[part] + up_near[part]
        found.append(mine if s == 0 else along(mine, s))
        passed.append(along_other(theirs, s))
    return join(at, found + passed)


def solution(mesh):
    grid = Mesh(mesh.devices.reshape(N, 2, N, N), ("x", "c", "y", "z"))
    return jax.shard_map(
        update,
        mesh=grid,
        in_specs=(P(("x", "c"), ("y", "z")), P()),
        out_specs=P(("x", "c"), ("y", "z"), None, None),
        check_vma=False,
    )
```

```python
import functools

import jax
import jax.numpy as jnp
from jax import lax
from jax.experimental import pallas as pl
from jax.experimental.pallas import tpu as pltpu
from jax.sharding import Mesh
from jax.sharding import PartitionSpec as P


N = 4
VMEM = pltpu.VMEM
SMEM = pltpu.SMEM
GRANT = 16 * 1024 * 1024


def move(value, target):
    pairs = []
    for c in range(2):
        for y in range(N):
            for z in range(N):
                core, gather, scatter = target(c, *((y, z) if c else (z, y)))
                to = (gather, scatter) if c else (scatter, gather)
                pairs.append(((c * N + y) * N + z, (core * N + to[0] % N) * N + to[1] % N))
    return lax.ppermute(value, ("c", "y", "z"), pairs)


def along(value, step):
    return move(value, lambda c, g, r: (c, g + step, r))


def across(value, step):
    return move(value, lambda c, g, r: (c, g, r + step))


def along_other(value, step):
    return move(value, lambda c, g, r: (1 - c, g + step, r))


def swap(value):
    return lax.ppermute(value, "c", [(0, 1), (1, 0)])


def hop(value, pairs):
    return lax.ppermute(value, "x", pairs)


def specs(space, count):
    return [pl.BlockSpec(memory_space=space)] * count


def cut_kernel(q, group, at_ref, slab_ref, *refs):
    for step in range(N):
        part = lax.rem(at_ref[1] + step, N)
        for block in range(2):
            start = pl.multiple_of((2 * block + at_ref[0]) * N * q + part * q, q)
            row = (2 * group + block) * q
            refs[step - N][row : row + q, :] = slab_ref[pl.ds(start, q), :]


def cut(at, slab, held):
    rows, inner = slab.shape
    q = rows // 16
    return pl.pallas_call(
        functools.partial(cut_kernel, q, 1 if held else 0),
        out_shape=[jax.ShapeDtypeStruct((4 * q, inner), slab.dtype)] * N,
        in_specs=specs(SMEM, 1) + specs(VMEM, 1 + len(held)),
        out_specs=specs(VMEM, N),
        input_output_aliases={2 + k: k for k in range(len(held))},
        compiler_params=pltpu.CompilerParams(vmem_limit_bytes=GRANT),
        cost_estimate=pl.CostEstimate(flops=10**6, bytes_accessed=3 * rows * inner * 4, transcendentals=0),
        name="cut",
    )(at, slab, *held)


def product_kernel(q, work, carried, groups, last, tab_ref, *refs):
    slabs = []
    for raw, places in work:
        count = len(groups) if raw else 1
        slabs.append((raw, refs[:count], list(zip(places, refs[count:]))))
        refs = refs[count + len(places) :]
    total_ref, refs = (refs[0], refs[1:]) if carried else (None, refs)
    raws = sum(raw for raw, _ in work)
    if last:
        (*outs, acc, b_parts, a_part), a_parts = refs, []
        a_parts.append(a_part)
    else:
        acc, a_parts, b_parts = refs[0], list(refs[1 : 1 + raws]), refs[-1]
    wide, side = 4 * q, 4 * q

    def halves(value, place, at):
        inner = value.shape[1]
        high = value.astype(jnp.bfloat16)
        place[at, :inner] = high
        place[at, inner:] = (value - high.astype(jnp.float32)).astype(jnp.bfloat16)

    terms = {}
    used = 0
    for raw, a_refs, pieces in slabs:
        if raw:
            parts, base = a_parts.pop(0), groups[0]
            rows = a_refs[0].shape[0]
            for k, ref in enumerate(a_refs):
                halves(ref[...], parts, slice(k * rows, (k + 1) * rows))
        else:
            parts, base = a_refs[0], 0
        for (place, row), ref in pieces:
            at = slice(wide * used, wide * (used + 1))
            halves(ref[row : row + wide, :], b_parts, at)
            terms.setdefault(place, []).append((parts, base, at))
            used += 1

    for n in range(4 * groups[0], 4 * groups[-1] + 4):
        to = n - 4 * groups[0] if last else n
        for place, pairs in terms.items():
            found = None
            for parts, base, at in pairs:
                inner = parts.shape[1] // 2
                column = (n - 4 * base) * side
                for left, right in ((0, 0), (0, 1), (1, 0)):
                    one = lax.dot_general(
                        b_parts[at, left * inner : (left + 1) * inner],
                        parts[column : column + side, right * inner : (right + 1) * inner],
                        (((1,), (1,)), ((), ())),
                        preferred_element_type=jnp.float32,
                    )
                    found = one if found is None else found + one
            rows = slice(wide * place, wide * (place + 1))
            if carried and place < 3:
                found = total_ref[n, rows, :] + found
            acc[to, rows, :] = found

    if last:
        offset = 0
        for ref in outs:
            first = (offset // 8 * 2 + groups[0]) * 8 + offset % 8

            def place(k, carry, ref=ref, first=first):
                code = tab_ref[first + k]
                safe = jnp.maximum(code, 0)
                start = pl.multiple_of((safe // 2) * q, q)
                for b in range(2):
                    tile = acc[(safe % 2) * 2 + b, pl.ds(start, q), :]
                    ref[k, :, b * side : (b + 1) * side] = jnp.where(code >= 0, tile, 0.0)
                return carry

            lax.fori_loop(0, ref.shape[0], place, 0, unroll=4)
            offset += ref.shape[0]


def product(tab, work, total, groups, sizes):
    args, form, raws, used = [tab], [], 0, 0
    for rows, slices in work:
        raw = rows[0].dtype == jnp.float32
        args += list(rows) + [piece for piece, _ in slices.values()]
        raws, used = raws + raw, used + len(slices)
        form.append((raw, tuple((place, row) for place, (_, row) in slices.items())))
    wide = next(iter(work[0][1].values()))[0].shape[1]
    q, rows, last = wide // 4, 4 * wide, bool(sizes)
    if total is not None:
        args.append(total)
    parts = (len(groups) * rows, 2 * wide)
    b_scratch = VMEM((wide * used, 2 * wide), jnp.bfloat16)
    if last:
        out_shape = [jax.ShapeDtypeStruct((k, q, rows // 2), jnp.float32) for k in sizes]
        scratch = [VMEM((4, rows, wide), jnp.float32), b_scratch, VMEM(parts, jnp.bfloat16)]
    else:
        out_shape = [jax.ShapeDtypeStruct((8, 3 * wide, wide), jnp.float32)]
        out_shape += [jax.ShapeDtypeStruct(parts, jnp.bfloat16)] * raws
        scratch = [b_scratch]
    return pl.pallas_call(
        functools.partial(product_kernel, q, form, total is not None, groups, last),
        out_shape=out_shape,
        in_specs=specs(SMEM, 1) + specs(VMEM, len(args) - 1),
        out_specs=specs(VMEM, len(out_shape)),
        scratch_shapes=scratch,
        input_output_aliases={} if last or total is None else {len(args) - 1: 0},
        compiler_params=pltpu.CompilerParams(vmem_limit_bytes=GRANT),
        cost_estimate=pl.CostEstimate(
            flops=12 * rows * rows * wide * len(groups), bytes_accessed=12 * rows * wide * 4, transcendentals=0
        ),
    )(*args)


def join_kernel(q, at_ref, *refs):
    pieces, out_ref, held = refs[:8], refs[8], refs[9]
    for index in range(8):
        kind = at_ref[0] if index < N else 1 - at_ref[0]
        mine = at_ref[1] if index < N else at_ref[2]
        part = lax.rem(mine + N - index % N, N)
        start = pl.multiple_of((kind * N + part) * q, q)
        for slot in range(2):
            held[slot, pl.ds(start, q), :] = pieces[index][slot]
    for slot in range(2):
        out_ref[0, slot] = held[slot].T


def join(at, pieces):
    _, q, half = pieces[0].shape
    return pl.pallas_call(
        functools.partial(join_kernel, q),
        out_shape=jax.ShapeDtypeStruct((1, 2, half, half), jnp.float32),
        in_specs=specs(SMEM, 1) + specs(VMEM, 8),
        out_specs=pl.BlockSpec(memory_space=VMEM),
        scratch_shapes=[VMEM((2, half, half), jnp.float32)],
        compiler_params=pltpu.CompilerParams(vmem_limit_bytes=GRANT),
        cost_estimate=pl.CostEstimate(flops=10**6, bytes_accessed=16 * half * half, transcendentals=0),
        name="join",
    )(at, *pieces)


def tile_codes(owner, x, c, gather, scatter):
    blocks = owner.shape[0]
    i = lax.broadcasted_iota(jnp.int32, (blocks, blocks), 0)
    j = lax.broadcasted_iota(jnp.int32, (blocks, blocks), 1)
    group = j // 2
    behind = (x - group // 2 + N) % N
    array = jnp.where(behind < 2, behind, 5 - behind) * 2 + jnp.where(group % 2 == c, 0, 1)
    code = jnp.where(j <= i, (array * 2 + j % 2) * 2 + i % 2 + 1, 0)
    index = jnp.arange(64, dtype=jnp.int32)
    far = (scatter + index // 16) % N
    mine = (index // 8) % 2
    near = (gather + (index // 2) % 4) % N
    wanted = jnp.where(c == 0, far * N + near, near * N + far) * 2 + index % 2
    wanted_group = 2 * x + jnp.where(mine == 0, c, 1 - c)
    hit = (owner[None] == wanted[:, None, None]) & ((i // 2)[None] == wanted_group[:, None, None])
    return jnp.sum(jnp.where(hit, code[None], 0), axis=(1, 2)) - 1


def update(panel, owner):
    x, c, y, z = (lax.axis_index(name) for name in "xcyz")
    gather, scatter = jnp.where(c == 0, z, y), jnp.where(c == 0, y, z)
    at = jnp.stack([c, gather, scatter]).astype(jnp.int32)
    tab = tile_codes(owner, x, c, gather, scatter)

    other = swap(panel)
    up, down = [along(panel, 1)], [along(panel, -1)]
    first, *sends = cut(at, other, cut(at, panel, []))
    small = [along(sends[s - 1], s) for s in range(1, N)]
    up.append(along(other, 1))
    down.append(along(other, -1))
    beyond = [along(up[0], 1), along(down[1], -1)]

    onward, wrap = [(0, 1), (1, 2), (2, 3)], [(0, 3)]
    both = jnp.concatenate([small[0], small[2]])
    a1, a3 = hop(first, onward), hop(first, wrap)
    b1, b3 = hop(both, onward), hop(both, wrap + [(1, 0)])
    c1, c3 = hop(small[1], onward), hop(small[1], wrap)
    a2, c2 = hop(a1, onward[1:]), hop(c1, onward[1:])
    b2 = hop(b3, wrap + [(3, 2)])

    wide = first.shape[0]
    low, high = [(v, 0) for v in (both, b1, b3, b2)], [(v, wide) for v in (both, b1, b3, b2)]
    zero, far = [(v, 0) for v in (first, a1, a3, a2)], [(v, 0) for v in (small[1], c1, c3, c2)]
    three, four = range(3), range(4)
    total, own_parts = product(tab, [((panel, other), dict(zip(three, zero)))], None, (0, 1), ())
    total, up_parts, down_parts = product(
        tab, [(up, dict(zip(three, low))), (down, dict(zip(three, high)))], total, (0, 1), ()
    )
    rest = [((own_parts,), {3: zero[3]}), ((up_parts,), {3: low[3]}), ((down_parts,), {3: high[3]})]
    own1, near1, far1, last1 = product(tab, [((beyond[1],), dict(zip(four, far)))] + rest, total, (1,), (8, 8, 8, 8))
    up_far, down_near = across(far1, 1), across(last1, -1)
    own0, near0, near0b, far0, last0 = product(
        tab, [((beyond[0],), dict(zip(four, far)))] + rest, total, (0,), (8, 4, 4, 8, 8)
    )
    down_far = across(far0, -1)
    up_near = across(near0, 1)
    up_sum = across(near1 + up_far, 1)
    up_near = [up_near, across(near0b, 1)]
    down_sum = across(last0 + down_far, -1)

    found, passed = [], []
    for s in range(N):
        part, piece = slice(2 * s, 2 * s + 2), slice(2 * (s % 2), 2 * (s % 2) + 2)
        theirs = own1[part] + up_sum[part] + down_near[part]
        mine = own0[part] + down_sum[part] + up_near[s // 2][piece]
        passed.append(along_other(theirs, s))
        found.append(mine if s == 0 else along(mine, s))
    return join(at, found + passed)


def solution(mesh):
    grid = Mesh(mesh.devices.reshape(N, 2, N, N), ("x", "c", "y", "z"))
    return jax.shard_map(
        update,
        mesh=grid,
        in_specs=(P(("x", "c"), ("y", "z")), P()),
        out_specs=P(("x", "c"), ("y", "z"), None, None),
        check_vma=False,
    )
```

```python
import functools

import jax
import jax.numpy as jnp
from jax import lax
from jax.experimental import pallas as pl
from jax.experimental.pallas import tpu as pltpu
from jax.sharding import Mesh
from jax.sharding import PartitionSpec as P


N = 4
VMEM = pltpu.VMEM
SMEM = pltpu.SMEM
GRANT = 16 * 1024 * 1024


def move(value, target):
    pairs = []
    for c in range(2):
        for y in range(N):
            for z in range(N):
                core, gather, scatter = target(c, *((y, z) if c else (z, y)))
                to = (gather, scatter) if c else (scatter, gather)
                pairs.append(((c * N + y) * N + z, (core * N + to[0] % N) * N + to[1] % N))
    return lax.ppermute(value, ("c", "y", "z"), pairs)


def along(value, step):
    return move(value, lambda c, g, r: (c, g + step, r))


def across(value, step):
    return move(value, lambda c, g, r: (c, g, r + step))


def along_other(value, step):
    return move(value, lambda c, g, r: (1 - c, g + step, r))


def swap(value):
    return lax.ppermute(value, "c", [(0, 1), (1, 0)])


def hop(value, pairs):
    return lax.ppermute(value, "x", pairs)


def specs(space, count):
    return [pl.BlockSpec(memory_space=space)] * count


def cut_kernel(q, group, at_ref, slab_ref, *refs):
    for step in range(N):
        part = lax.rem(at_ref[1] + step, N)
        for block in range(2):
            start = pl.multiple_of((2 * block + at_ref[0]) * N * q + part * q, q)
            row = (2 * group + block) * q
            refs[step - N][row : row + q, :] = slab_ref[pl.ds(start, q), :]


def cut(at, slab, held):
    rows, inner = slab.shape
    q = rows // 16
    return pl.pallas_call(
        functools.partial(cut_kernel, q, 1 if held else 0),
        out_shape=[jax.ShapeDtypeStruct((4 * q, inner), slab.dtype)] * N,
        in_specs=specs(SMEM, 1) + specs(VMEM, 1 + len(held)),
        out_specs=specs(VMEM, N),
        input_output_aliases={2 + k: k for k in range(len(held))},
        compiler_params=pltpu.CompilerParams(vmem_limit_bytes=GRANT),
        cost_estimate=pl.CostEstimate(flops=10**6, bytes_accessed=3 * rows * inner * 4, transcendentals=0),
        name="cut",
    )(at, slab, *held)


def product_kernel(q, work, carried, groups, last, tab_ref, *refs):
    slabs = []
    for raw, places in work:
        count = len(groups) if raw else 1
        slabs.append((raw, refs[:count], list(zip(places, refs[count:]))))
        refs = refs[count + len(places) :]
    total_ref, refs = (refs[0], refs[1:]) if carried else (None, refs)
    raws = sum(raw for raw, _ in work)
    if last:
        (*outs, acc, b_parts, a_part), a_parts = refs, []
        a_parts.append(a_part)
    else:
        acc, a_parts, b_parts = refs[0], list(refs[1 : 1 + raws]), refs[-1]
    wide, side = 4 * q, 4 * q

    def halves(value, place, at):
        inner = value.shape[1]
        high = value.astype(jnp.bfloat16)
        place[at, :inner] = high
        place[at, inner:] = (value - high.astype(jnp.float32)).astype(jnp.bfloat16)

    terms = {}
    used = 0
    for raw, a_refs, pieces in slabs:
        if raw:
            parts, base = a_parts.pop(0), groups[0]
            rows = a_refs[0].shape[0]
            for k, ref in enumerate(a_refs):
                halves(ref[...], parts, slice(k * rows, (k + 1) * rows))
        else:
            parts, base = a_refs[0], 0
        for (place, row), ref in pieces:
            at = slice(wide * used, wide * (used + 1))
            halves(ref[row : row + wide, :], b_parts, at)
            terms.setdefault(place, []).append((parts, base, at))
            used += 1

    for n in range(4 * groups[0], 4 * groups[-1] + 4):
        to = n - 4 * groups[0] if last else n
        for place, pairs in terms.items():
            found = None
            for parts, base, at in pairs:
                inner = parts.shape[1] // 2
                column = (n - 4 * base) * side
                for left, right in ((0, 0), (0, 1), (1, 0)):
                    one = lax.dot_general(
                        b_parts[at, left * inner : (left + 1) * inner],
                        parts[column : column + side, right * inner : (right + 1) * inner],
                        (((1,), (1,)), ((), ())),
                        preferred_element_type=jnp.float32,
                    )
                    found = one if found is None else found + one
            rows = slice(wide * place, wide * (place + 1))
            if carried and place < 3:
                found = total_ref[n, rows, :] + found
            acc[to, rows, :] = found

    if last:
        offset = 0
        for ref in outs:
            first = (offset // 8 * 2 + groups[0]) * 8 + offset % 8

            def place(k, carry, ref=ref, first=first):
                code = tab_ref[first + k]
                safe = jnp.maximum(code, 0)
                start = pl.multiple_of((safe // 2) * q, q)
                for b in range(2):
                    tile = acc[(safe % 2) * 2 + b, pl.ds(start, q), :]
                    ref[k, :, b * side : (b + 1) * side] = jnp.where(code >= 0, tile, 0.0)
                return carry

            lax.fori_loop(0, ref.shape[0], place, 0, unroll=4)
            offset += ref.shape[0]


def product(tab, work, total, groups, sizes):
    args, form, raws, used = [tab], [], 0, 0
    for rows, slices in work:
        raw = rows[0].dtype == jnp.float32
        args += list(rows) + [piece for piece, _ in slices.values()]
        raws, used = raws + raw, used + len(slices)
        form.append((raw, tuple((place, row) for place, (_, row) in slices.items())))
    wide = next(iter(work[0][1].values()))[0].shape[1]
    q, rows, last = wide // 4, 4 * wide, bool(sizes)
    if total is not None:
        args.append(total)
    parts = (len(groups) * rows, 2 * wide)
    b_scratch = VMEM((wide * used, 2 * wide), jnp.bfloat16)
    if last:
        out_shape = [jax.ShapeDtypeStruct((k, q, rows // 2), jnp.float32) for k in sizes]
        scratch = [VMEM((4, rows, wide), jnp.float32), b_scratch, VMEM(parts, jnp.bfloat16)]
    else:
        out_shape = [jax.ShapeDtypeStruct((8, 3 * wide, wide), jnp.float32)]
        out_shape += [jax.ShapeDtypeStruct(parts, jnp.bfloat16)] * raws
        scratch = [b_scratch]
    return pl.pallas_call(
        functools.partial(product_kernel, q, form, total is not None, groups, last),
        out_shape=out_shape,
        in_specs=specs(SMEM, 1) + specs(VMEM, len(args) - 1),
        out_specs=specs(VMEM, len(out_shape)),
        scratch_shapes=scratch,
        input_output_aliases={} if last or total is None else {len(args) - 1: 0},
        compiler_params=pltpu.CompilerParams(vmem_limit_bytes=GRANT),
        cost_estimate=pl.CostEstimate(
            flops=12 * rows * rows * wide * len(groups), bytes_accessed=12 * rows * wide * 4, transcendentals=0
        ),
    )(*args)


def join_kernel(q, at_ref, *refs):
    pieces, out_ref, held = refs[:8], refs[8], refs[9]
    for index in range(8):
        kind = at_ref[0] if index < N else 1 - at_ref[0]
        mine = at_ref[1] if index < N else at_ref[2]
        part = lax.rem(mine + N - index % N, N)
        start = pl.multiple_of((kind * N + part) * q, q)
        for slot in range(2):
            held[slot, pl.ds(start, q), :] = pieces[index][slot]
    for slot in range(2):
        out_ref[0, slot] = held[slot].T


def join(at, pieces):
    _, q, half = pieces[0].shape
    return pl.pallas_call(
        functools.partial(join_kernel, q),
        out_shape=jax.ShapeDtypeStruct((1, 2, half, half), jnp.float32),
        in_specs=specs(SMEM, 1) + specs(VMEM, 8),
        out_specs=pl.BlockSpec(memory_space=VMEM),
        scratch_shapes=[VMEM((2, half, half), jnp.float32)],
        compiler_params=pltpu.CompilerParams(vmem_limit_bytes=GRANT),
        cost_estimate=pl.CostEstimate(flops=10**6, bytes_accessed=16 * half * half, transcendentals=0),
        name="join",
    )(at, *pieces)


def tile_codes(owner, x, c, gather, scatter):
    blocks = owner.shape[0]
    i = lax.broadcasted_iota(jnp.int32, (blocks, blocks), 0)
    j = lax.broadcasted_iota(jnp.int32, (blocks, blocks), 1)
    group = j // 2
    behind = (x - group // 2 + N) % N
    array = jnp.where(behind < 2, behind, 5 - behind) * 2 + jnp.where(group % 2 == c, 0, 1)
    code = jnp.where(j <= i, (array * 2 + j % 2) * 2 + i % 2 + 1, 0)
    index = jnp.arange(64, dtype=jnp.int32)
    far = (scatter + index // 16) % N
    mine = (index // 8) % 2
    near = (gather + (index // 2) % 4) % N
    wanted = jnp.where(c == 0, far * N + near, near * N + far) * 2 + index % 2
    wanted_group = 2 * x + jnp.where(mine == 0, c, 1 - c)
    hit = (owner[None] == wanted[:, None, None]) & ((i // 2)[None] == wanted_group[:, None, None])
    return jnp.sum(jnp.where(hit, code[None], 0), axis=(1, 2)) - 1


def update(panel, owner):
    x, c, y, z = (lax.axis_index(name) for name in "xcyz")
    gather, scatter = jnp.where(c == 0, z, y), jnp.where(c == 0, y, z)
    at = jnp.stack([c, gather, scatter]).astype(jnp.int32)
    tab = tile_codes(owner, x, c, gather, scatter)

    other = swap(panel)
    up, down = [along(panel, 1)], [along(panel, -1)]
    first, *sends = cut(at, other, cut(at, panel, []))
    small = [along(sends[s - 1], s) for s in range(1, N)]
    up.append(along(other, 1))
    down.append(along(other, -1))
    beyond = [along(up[0], 1), along(down[1], -1)]

    onward, wrap = [(0, 1), (1, 2), (2, 3)], [(0, 3)]
    both = jnp.concatenate([small[0], small[2]])
    a1, a3 = hop(first, onward), hop(first, wrap + [(1, 0)])
    b1, b3 = hop(both, onward), hop(both, wrap)
    c1, c3 = hop(small[1], onward), hop(small[1], wrap + [(1, 0)])
    a2, c2 = hop(a3, wrap + [(3, 2)]), hop(c3, wrap + [(3, 2)])
    b2 = hop(b1, onward[1:])

    wide = first.shape[0]
    low, high = [(v, 0) for v in (both, b1, b3, b2)], [(v, wide) for v in (both, b1, b3, b2)]
    zero, far = [(v, 0) for v in (first, a1, a3, a2)], [(v, 0) for v in (small[1], c1, c3, c2)]
    three, four = range(3), range(4)
    total, own_parts = product(tab, [((panel, other), dict(zip(three, zero)))], None, (0, 1), ())
    total, up_parts, down_parts = product(
        tab, [(up, dict(zip(three, low))), (down, dict(zip(three, high)))], total, (0, 1), ()
    )
    rest = [((own_parts,), {3: zero[3]}), ((up_parts,), {3: low[3]}), ((down_parts,), {3: high[3]})]
    own0, near0, far0, last0 = product(tab, [((beyond[0],), dict(zip(four, far)))] + rest, total, (0,), (8, 8, 8, 8))
    up_far, down_near = across(far0, 1), across(last0, -1)
    own1, near1, far1, last1 = product(tab, [((beyond[1],), dict(zip(four, far)))] + rest, total, (1,), (8, 8, 8, 8))
    down_far = across(far1, -1)
    up_near = across(near1, 1)
    up_sum = across(near0 + up_far, 1)
    down_sum = across(last1 + down_far, -1)

    found, passed = [], []
    for s in range(N):
        part = slice(2 * s, 2 * s + 2)
        mine = own0[part] + up_sum[part] + down_near[part]
        theirs = own1[part] + down_sum[part] + up_near[part]
        found.append(mine if s == 0 else along(mine, s))
        passed.append(along_other(theirs, s))
    return join(at, found + passed)


def solution(mesh):
    grid = Mesh(mesh.devices.reshape(N, 2, N, N), ("x", "c", "y", "z"))
    return jax.shard_map(
        update,
        mesh=grid,
        in_specs=(P(("x", "c"), ("y", "z")), P()),
        out_specs=P(("x", "c"), ("y", "z"), None, None),
        check_vma=False,
    )
```

```python
import functools

import jax
import jax.numpy as jnp
from jax import lax
from jax.experimental import pallas as pl
from jax.experimental.pallas import tpu as pltpu
from jax.sharding import Mesh
from jax.sharding import PartitionSpec as P


N = 4
VMEM = pltpu.VMEM
SMEM = pltpu.SMEM
GRANT = 16 * 1024 * 1024


def move(value, target):
    pairs = []
    for c in range(2):
        for y in range(N):
            for z in range(N):
                core, gather, scatter = target(c, *((y, z) if c else (z, y)))
                to = (gather, scatter) if c else (scatter, gather)
                pairs.append(((c * N + y) * N + z, (core * N + to[0] % N) * N + to[1] % N))
    return lax.ppermute(value, ("c", "y", "z"), pairs)


def along(value, step):
    return move(value, lambda c, g, r: (c, g + step, r))


def across(value, step):
    return move(value, lambda c, g, r: (c, g, r + step))


def along_other(value, step):
    return move(value, lambda c, g, r: (1 - c, g + step, r))


def swap(value):
    return lax.ppermute(value, "c", [(0, 1), (1, 0)])


def hop(value, pairs):
    return lax.ppermute(value, "x", pairs)


def specs(space, count):
    return [pl.BlockSpec(memory_space=space)] * count


def cut_kernel(q, group, at_ref, slab_ref, *refs):
    for step in range(N):
        part = lax.rem(at_ref[1] + step, N)
        for block in range(2):
            start = pl.multiple_of((2 * block + at_ref[0]) * N * q + part * q, q)
            row = (2 * group + block) * q
            refs[step - N][row : row + q, :] = slab_ref[pl.ds(start, q), :]


def cut(at, slab, held):
    rows, inner = slab.shape
    q = rows // 16
    return pl.pallas_call(
        functools.partial(cut_kernel, q, 1 if held else 0),
        out_shape=[jax.ShapeDtypeStruct((4 * q, inner), slab.dtype)] * N,
        in_specs=specs(SMEM, 1) + specs(VMEM, 1 + len(held)),
        out_specs=specs(VMEM, N),
        input_output_aliases={2 + k: k for k in range(len(held))},
        compiler_params=pltpu.CompilerParams(vmem_limit_bytes=GRANT),
        cost_estimate=pl.CostEstimate(flops=10**6, bytes_accessed=3 * rows * inner * 4, transcendentals=0),
        name="cut",
    )(at, slab, *held)


def product_kernel(q, work, carried, groups, last, tab_ref, *refs):
    slabs = []
    for raw, places in work:
        count = len(groups) if raw else 1
        slabs.append((raw, refs[:count], list(zip(places, refs[count:]))))
        refs = refs[count + len(places) :]
    total_ref, refs = (refs[0], refs[1:]) if carried else (None, refs)
    raws = sum(raw for raw, _ in work)
    if last:
        (*outs, acc, b_parts, a_part), a_parts = refs, []
        a_parts.append(a_part)
    else:
        acc, a_parts, b_parts = refs[0], list(refs[1 : 1 + raws]), refs[-1]
    wide, side = 4 * q, 4 * q

    def halves(value, place, at):
        inner = value.shape[1]
        high = value.astype(jnp.bfloat16)
        place[at, :inner] = high
        place[at, inner:] = (value - high.astype(jnp.float32)).astype(jnp.bfloat16)

    terms = {}
    used = 0
    for raw, a_refs, pieces in slabs:
        if raw:
            parts, base = a_parts.pop(0), groups[0]
            rows = a_refs[0].shape[0]
            for k, ref in enumerate(a_refs):
                halves(ref[...], parts, slice(k * rows, (k + 1) * rows))
        else:
            parts, base = a_refs[0], 0
        for (place, row), ref in pieces:
            at = slice(wide * used, wide * (used + 1))
            halves(ref[row : row + wide, :], b_parts, at)
            terms.setdefault(place, []).append((parts, base, at))
            used += 1

    for n in range(4 * groups[0], 4 * groups[-1] + 4):
        to = n - 4 * groups[0] if last else n
        for place, pairs in terms.items():
            found = None
            for parts, base, at in pairs:
                inner = parts.shape[1] // 2
                column = (n - 4 * base) * side
                for left, right in ((0, 0), (0, 1), (1, 0)):
                    one = lax.dot_general(
                        b_parts[at, left * inner : (left + 1) * inner],
                        parts[column : column + side, right * inner : (right + 1) * inner],
                        (((1,), (1,)), ((), ())),
                        preferred_element_type=jnp.float32,
                    )
                    found = one if found is None else found + one
            rows = slice(wide * place, wide * (place + 1))
            if carried and place < 3:
                found = total_ref[n, rows, :] + found
            acc[to, rows, :] = found

    if last:
        offset = 0
        for ref in outs:
            first = (offset // 8 * 2 + groups[0]) * 8 + offset % 8

            def place(k, carry, ref=ref, first=first):
                code = tab_ref[first + k]
                safe = jnp.maximum(code, 0)
                start = pl.multiple_of((safe // 2) * q, q)
                for b in range(2):
                    tile = acc[(safe % 2) * 2 + b, pl.ds(start, q), :]
                    ref[k, :, b * side : (b + 1) * side] = jnp.where(code >= 0, tile, 0.0)
                return carry

            lax.fori_loop(0, ref.shape[0], place, 0, unroll=4)
            offset += ref.shape[0]


def product(tab, work, total, groups, sizes):
    args, form, raws, used = [tab], [], 0, 0
    for rows, slices in work:
        raw = rows[0].dtype == jnp.float32
        args += list(rows) + [piece for piece, _ in slices.values()]
        raws, used = raws + raw, used + len(slices)
        form.append((raw, tuple((place, row) for place, (_, row) in slices.items())))
    wide = next(iter(work[0][1].values()))[0].shape[1]
    q, rows, last = wide // 4, 4 * wide, bool(sizes)
    if total is not None:
        args.append(total)
    parts = (len(groups) * rows, 2 * wide)
    b_scratch = VMEM((wide * used, 2 * wide), jnp.bfloat16)
    if last:
        out_shape = [jax.ShapeDtypeStruct((k, q, rows // 2), jnp.float32) for k in sizes]
        scratch = [VMEM((4, rows, wide), jnp.float32), b_scratch, VMEM(parts, jnp.bfloat16)]
    else:
        out_shape = [jax.ShapeDtypeStruct((8, 3 * wide, wide), jnp.float32)]
        out_shape += [jax.ShapeDtypeStruct(parts, jnp.bfloat16)] * raws
        scratch = [b_scratch]
    return pl.pallas_call(
        functools.partial(product_kernel, q, form, total is not None, groups, last),
        out_shape=out_shape,
        in_specs=specs(SMEM, 1) + specs(VMEM, len(args) - 1),
        out_specs=specs(VMEM, len(out_shape)),
        scratch_shapes=scratch,
        input_output_aliases={} if last or total is None else {len(args) - 1: 0},
        compiler_params=pltpu.CompilerParams(vmem_limit_bytes=GRANT),
        cost_estimate=pl.CostEstimate(
            flops=12 * rows * rows * wide * len(groups), bytes_accessed=12 * rows * wide * 4, transcendentals=0
        ),
    )(*args)


def join_kernel(q, at_ref, *refs):
    pieces, out_ref, held = refs[:8], refs[8], refs[9]
    for index in range(8):
        kind = at_ref[0] if index < N else 1 - at_ref[0]
        mine = at_ref[1] if index < N else at_ref[2]
        part = lax.rem(mine + N - index % N, N)
        start = pl.multiple_of((kind * N + part) * q, q)
        for slot in range(2):
            held[slot, pl.ds(start, q), :] = pieces[index][slot]
    for slot in range(2):
        out_ref[0, slot] = held[slot].T


def join(at, pieces):
    _, q, half = pieces[0].shape
    return pl.pallas_call(
        functools.partial(join_kernel, q),
        out_shape=jax.ShapeDtypeStruct((1, 2, half, half), jnp.float32),
        in_specs=specs(SMEM, 1) + specs(VMEM, 8),
        out_specs=pl.BlockSpec(memory_space=VMEM),
        scratch_shapes=[VMEM((2, half, half), jnp.float32)],
        compiler_params=pltpu.CompilerParams(vmem_limit_bytes=GRANT),
        cost_estimate=pl.CostEstimate(flops=10**6, bytes_accessed=16 * half * half, transcendentals=0),
        name="join",
    )(at, *pieces)


def tile_codes(owner, x, c, gather, scatter):
    blocks = owner.shape[0]
    i = lax.broadcasted_iota(jnp.int32, (blocks, blocks), 0)
    j = lax.broadcasted_iota(jnp.int32, (blocks, blocks), 1)
    group = j // 2
    behind = (x - group // 2 + N) % N
    array = jnp.where(behind < 2, behind, 5 - behind) * 2 + jnp.where(group % 2 == c, 0, 1)
    code = jnp.where(j <= i, (array * 2 + j % 2) * 2 + i % 2 + 1, 0)
    index = jnp.arange(64, dtype=jnp.int32)
    far = (scatter + index // 16) % N
    mine = (index // 8) % 2
    near = (gather + (index // 2) % 4) % N
    wanted = jnp.where(c == 0, far * N + near, near * N + far) * 2 + index % 2
    wanted_group = 2 * x + jnp.where(mine == 0, c, 1 - c)
    hit = (owner[None] == wanted[:, None, None]) & ((i // 2)[None] == wanted_group[:, None, None])
    return jnp.sum(jnp.where(hit, code[None], 0), axis=(1, 2)) - 1


def update(panel, owner):
    x, c, y, z = (lax.axis_index(name) for name in "xcyz")
    gather, scatter = jnp.where(c == 0, z, y), jnp.where(c == 0, y, z)
    at = jnp.stack([c, gather, scatter]).astype(jnp.int32)
    tab = tile_codes(owner, x, c, gather, scatter)

    other = swap(panel)
    up, down = [along(panel, 1)], [along(panel, -1)]
    first, *sends = cut(at, other, cut(at, panel, []))
    small = [along(sends[s - 1], s) for s in range(1, N)]
    up.append(along(other, 1))
    down.append(along(other, -1))
    beyond = [along(up[0], 1), along(down[1], -1)]

    onward, wrap = [(0, 1), (1, 2), (2, 3)], [(0, 3)]
    both = jnp.concatenate([small[0], small[2]])
    a1, a3 = hop(first, onward), hop(first, wrap)
    b1, b3 = hop(both, onward), hop(both, wrap)
    c1, c3 = hop(small[1], onward), hop(small[1], wrap)
    d2 = hop(jnp.concatenate([first, small[1]]), [(0, 2), (1, 3)])
    b2 = hop(b1, onward[1:])

    wide = first.shape[0]
    low, high = [(v, 0) for v in (both, b1, b3, b2)], [(v, wide) for v in (both, b1, b3, b2)]
    zero, far = [(first, 0), (a1, 0), (a3, 0), (d2, 0)], [(small[1], 0), (c1, 0), (c3, 0), (d2, wide)]
    three, four = range(3), range(4)
    total, own_parts = product(tab, [((panel, other), dict(zip(three, zero)))], None, (0, 1), ())
    total, up_parts, down_parts = product(
        tab, [(up, dict(zip(three, low))), (down, dict(zip(three, high)))], total, (0, 1), ()
    )
    rest = [((own_parts,), {3: zero[3]}), ((up_parts,), {3: low[3]}), ((down_parts,), {3: high[3]})]
    own0, near0, far0, last0 = product(tab, [((beyond[0],), dict(zip(four, far)))] + rest, total, (0,), (8, 8, 8, 8))
    up_far, down_near = across(far0, 1), across(last0, -1)
    own1, near1, far1, last1 = product(tab, [((beyond[1],), dict(zip(four, far)))] + rest, total, (1,), (8, 8, 8, 8))
    down_far = across(far1, -1)
    up_near = across(near1, 1)
    up_sum = across(near0 + up_far, 1)
    down_sum = across(last1 + down_far, -1)

    found, passed = [], []
    for s in range(N):
        part = slice(2 * s, 2 * s + 2)
        mine = own0[part] + up_sum[part] + down_near[part]
        theirs = own1[part] + down_sum[part] + up_near[part]
        found.append(mine if s == 0 else along(mine, s))
        passed.append(along_other(theirs, s))
    return join(at, found + passed)


def solution(mesh):
    grid = Mesh(mesh.devices.reshape(N, 2, N, N), ("x", "c", "y", "z"))
    return jax.shard_map(
        update,
        mesh=grid,
        in_specs=(P(("x", "c"), ("y", "z")), P()),
        out_specs=P(("x", "c"), ("y", "z"), None, None),
        check_vma=False,
    )
```

```python
import functools

import jax
import jax.numpy as jnp
from jax import lax
from jax.experimental import pallas as pl
from jax.experimental.pallas import tpu as pltpu
from jax.sharding import Mesh
from jax.sharding import PartitionSpec as P


N = 4
VMEM = pltpu.VMEM
SMEM = pltpu.SMEM
GRANT = 16 * 1024 * 1024


def move(value, target):
    pairs = []
    for c in range(2):
        for y in range(N):
            for z in range(N):
                core, gather, scatter = target(c, *((y, z) if c else (z, y)))
                to = (gather, scatter) if c else (scatter, gather)
                pairs.append(((c * N + y) * N + z, (core * N + to[0] % N) * N + to[1] % N))
    return lax.ppermute(value, ("c", "y", "z"), pairs)


def along(value, step):
    return move(value, lambda c, g, r: (c, g + step, r))


def across(value, step):
    return move(value, lambda c, g, r: (c, g, r + step))


def along_other(value, step):
    return move(value, lambda c, g, r: (1 - c, g + step, r))


def swap(value):
    return lax.ppermute(value, "c", [(0, 1), (1, 0)])


def hop(value, pairs):
    return lax.ppermute(value, "x", pairs)


def specs(space, count):
    return [pl.BlockSpec(memory_space=space)] * count


def cut_kernel(q, group, at_ref, slab_ref, *refs):
    for step in range(N):
        part = lax.rem(at_ref[1] + step, N)
        for block in range(2):
            start = pl.multiple_of((2 * block + at_ref[0]) * N * q + part * q, q)
            row = (2 * group + block) * q
            refs[step - N][row : row + q, :] = slab_ref[pl.ds(start, q), :]


def cut(at, slab, held):
    rows, inner = slab.shape
    q = rows // 16
    return pl.pallas_call(
        functools.partial(cut_kernel, q, 1 if held else 0),
        out_shape=[jax.ShapeDtypeStruct((4 * q, inner), slab.dtype)] * N,
        in_specs=specs(SMEM, 1) + specs(VMEM, 1 + len(held)),
        out_specs=specs(VMEM, N),
        input_output_aliases={2 + k: k for k in range(len(held))},
        compiler_params=pltpu.CompilerParams(vmem_limit_bytes=GRANT),
        cost_estimate=pl.CostEstimate(flops=10**6, bytes_accessed=3 * rows * inner * 4, transcendentals=0),
        name="cut",
    )(at, slab, *held)


def product_kernel(q, work, carried, groups, last, tab_ref, *refs):
    slabs = []
    for raw, places in work:
        count = len(groups) if raw else 1
        slabs.append((raw, refs[:count], list(zip(places, refs[count:]))))
        refs = refs[count + len(places) :]
    total_ref, refs = (refs[0], refs[1:]) if carried else (None, refs)
    raws = sum(raw for raw, _ in work)
    if last:
        (*outs, acc, b_parts, a_part), a_parts = refs, []
        a_parts.append(a_part)
    else:
        acc, a_parts, b_parts = refs[0], list(refs[1 : 1 + raws]), refs[-1]
    wide, side = 4 * q, 4 * q

    def halves(value, place, at):
        inner = value.shape[1]
        high = value.astype(jnp.bfloat16)
        place[at, :inner] = high
        place[at, inner:] = (value - high.astype(jnp.float32)).astype(jnp.bfloat16)

    terms = {}
    used = 0
    for raw, a_refs, pieces in slabs:
        if raw:
            parts, base = a_parts.pop(0), groups[0]
            rows = a_refs[0].shape[0]
            for k, ref in enumerate(a_refs):
                halves(ref[...], parts, slice(k * rows, (k + 1) * rows))
        else:
            parts, base = a_refs[0], 0
        for (place, row), ref in pieces:
            at = slice(wide * used, wide * (used + 1))
            halves(ref[row : row + wide, :], b_parts, at)
            terms.setdefault(place, []).append((parts, base, at))
            used += 1

    for n in range(4 * groups[0], 4 * groups[-1] + 4):
        to = n - 4 * groups[0] if last else n
        for place, pairs in terms.items():
            found = None
            for parts, base, at in pairs:
                inner = parts.shape[1] // 2
                column = (n - 4 * base) * side
                for left, right in ((0, 0), (0, 1), (1, 0)):
                    one = lax.dot_general(
                        b_parts[at, left * inner : (left + 1) * inner],
                        parts[column : column + side, right * inner : (right + 1) * inner],
                        (((1,), (1,)), ((), ())),
                        preferred_element_type=jnp.float32,
                    )
                    found = one if found is None else found + one
            rows = slice(wide * place, wide * (place + 1))
            if carried and place < 3:
                found = total_ref[n, rows, :] + found
            acc[to, rows, :] = found

    if last:
        offset = 0
        for ref in outs:
            first = (offset // 8 * 2 + groups[0]) * 8 + offset % 8

            def place(k, carry, ref=ref, first=first):
                code = tab_ref[first + k]
                safe = jnp.maximum(code, 0)
                start = pl.multiple_of((safe // 2) * q, q)
                for b in range(2):
                    tile = acc[(safe % 2) * 2 + b, pl.ds(start, q), :]
                    ref[k, :, b * side : (b + 1) * side] = jnp.where(code >= 0, tile, 0.0)
                return carry

            lax.fori_loop(0, ref.shape[0], place, 0, unroll=4)
            offset += ref.shape[0]


def product(tab, work, total, groups, sizes):
    args, form, raws, used = [tab], [], 0, 0
    for rows, slices in work:
        raw = rows[0].dtype == jnp.float32
        args += list(rows) + [piece for piece, _ in slices.values()]
        raws, used = raws + raw, used + len(slices)
        form.append((raw, tuple((place, row) for place, (_, row) in slices.items())))
    wide = next(iter(work[0][1].values()))[0].shape[1]
    q, rows, last = wide // 4, 4 * wide, bool(sizes)
    if total is not None:
        args.append(total)
    parts = (len(groups) * rows, 2 * wide)
    b_scratch = VMEM((wide * used, 2 * wide), jnp.bfloat16)
    if last:
        out_shape = [jax.ShapeDtypeStruct((k, q, rows // 2), jnp.float32) for k in sizes]
        scratch = [VMEM((4, rows, wide), jnp.float32), b_scratch, VMEM(parts, jnp.bfloat16)]
    else:
        out_shape = [jax.ShapeDtypeStruct((8, 3 * wide, wide), jnp.float32)]
        out_shape += [jax.ShapeDtypeStruct(parts, jnp.bfloat16)] * raws
        scratch = [b_scratch]
    return pl.pallas_call(
        functools.partial(product_kernel, q, form, total is not None, groups, last),
        out_shape=out_shape,
        in_specs=specs(SMEM, 1) + specs(VMEM, len(args) - 1),
        out_specs=specs(VMEM, len(out_shape)),
        scratch_shapes=scratch,
        input_output_aliases={} if last or total is None else {len(args) - 1: 0},
        compiler_params=pltpu.CompilerParams(vmem_limit_bytes=GRANT),
        cost_estimate=pl.CostEstimate(
            flops=12 * rows * rows * wide * len(groups), bytes_accessed=12 * rows * wide * 4, transcendentals=0
        ),
    )(*args)


def join_kernel(q, at_ref, *refs):
    pieces, out_ref, held = refs[:8], refs[8], refs[9]
    for index in range(8):
        kind = at_ref[0] if index < N else 1 - at_ref[0]
        mine = at_ref[1] if index < N else at_ref[2]
        part = lax.rem(mine + N - index % N, N)
        start = pl.multiple_of((kind * N + part) * q, q)
        for slot in range(2):
            held[slot, pl.ds(start, q), :] = pieces[index][slot]
    for slot in range(2):
        out_ref[0, slot] = held[slot].T


def join(at, pieces):
    _, q, half = pieces[0].shape
    return pl.pallas_call(
        functools.partial(join_kernel, q),
        out_shape=jax.ShapeDtypeStruct((1, 2, half, half), jnp.float32),
        in_specs=specs(SMEM, 1) + specs(VMEM, 8),
        out_specs=pl.BlockSpec(memory_space=VMEM),
        scratch_shapes=[VMEM((2, half, half), jnp.float32)],
        compiler_params=pltpu.CompilerParams(vmem_limit_bytes=GRANT),
        cost_estimate=pl.CostEstimate(flops=10**6, bytes_accessed=16 * half * half, transcendentals=0),
        name="join",
    )(at, *pieces)


def tile_codes(owner, x, c, gather, scatter):
    blocks = owner.shape[0]
    i = lax.broadcasted_iota(jnp.int32, (blocks, blocks), 0)
    j = lax.broadcasted_iota(jnp.int32, (blocks, blocks), 1)
    group = j // 2
    behind = (x - group // 2 + N) % N
    array = jnp.where(behind < 2, behind, 5 - behind) * 2 + jnp.where(group % 2 == c, 0, 1)
    code = jnp.where(j <= i, (array * 2 + j % 2) * 2 + i % 2 + 1, 0)
    index = jnp.arange(64, dtype=jnp.int32)
    far = (scatter + index // 16) % N
    mine = (index // 8) % 2
    near = (gather + (index // 2) % 4) % N
    wanted = jnp.where(c == 0, far * N + near, near * N + far) * 2 + index % 2
    wanted_group = 2 * x + jnp.where(mine == 0, c, 1 - c)
    hit = (owner[None] == wanted[:, None, None]) & ((i // 2)[None] == wanted_group[:, None, None])
    return jnp.sum(jnp.where(hit, code[None], 0), axis=(1, 2)) - 1


def update(panel, owner):
    x, c, y, z = (lax.axis_index(name) for name in "xcyz")
    gather, scatter = jnp.where(c == 0, z, y), jnp.where(c == 0, y, z)
    at = jnp.stack([c, gather, scatter]).astype(jnp.int32)
    tab = tile_codes(owner, x, c, gather, scatter)

    other = swap(panel)
    up, down = [along(panel, 1)], [along(panel, -1)]
    first, *sends = cut(at, other, cut(at, panel, []))
    small = [along(sends[s - 1], s) for s in range(1, N)]
    up.append(along(other, 1))
    down.append(along(other, -1))
    beyond = [along(up[0], 1), along(down[1], -1)]

    onward, wrap = [(0, 1), (1, 2), (2, 3)], [(0, 3)]
    both = jnp.concatenate([small[0], small[2]])
    a1, a3 = hop(first, onward), hop(first, wrap)
    b1, b3 = hop(both, onward), hop(both, wrap + [(1, 0)])
    c1, c3 = hop(small[1], onward), hop(small[1], wrap)
    a2, c2 = hop(a1, onward[1:]), hop(c1, onward[1:])
    b2 = hop(b3, wrap + [(3, 2)])

    wide = first.shape[0]
    low, high = [(v, 0) for v in (both, b1, b3, b2)], [(v, wide) for v in (both, b1, b3, b2)]
    zero, far = [(v, 0) for v in (first, a1, a3, a2)], [(v, 0) for v in (small[1], c1, c3, c2)]
    three, four = range(3), range(4)
    total, own_parts = product(tab, [((panel, other), dict(zip(three, zero)))], None, (0, 1), ())
    total, up_parts, down_parts = product(
        tab, [(up, dict(zip(three, low))), (down, dict(zip(three, high)))], total, (0, 1), ()
    )
    rest = [((own_parts,), {3: zero[3]}), ((up_parts,), {3: low[3]}), ((down_parts,), {3: high[3]})]
    own0, near0, far0, last0 = product(tab, [((beyond[0],), dict(zip(four, far)))] + rest, total, (0,), (8, 8, 8, 8))
    up_far, down_near = across(far0, 1), across(last0, -1)
    own1, near1, far1, last1 = product(tab, [((beyond[1],), dict(zip(four, far)))] + rest, total, (1,), (8, 8, 8, 8))
    down_far = across(far1, -1)
    up_near = across(near1, 1)
    up_sum = across(near0 + up_far, 1)
    down_sum = across(last1 + down_far, -1)

    found, passed = [], []
    for s in range(N):
        part = slice(2 * s, 2 * s + 2)
        mine = own0[part] + up_sum[part] + down_near[part]
        theirs = own1[part] + down_sum[part] + up_near[part]
        found.append(mine if s == 0 else along(mine, s))
        passed.append(along_other(theirs, s))
    return join(at, found + passed)


def solution(mesh):
    grid = Mesh(mesh.devices.reshape(N, 2, N, N), ("x", "c", "y", "z"))
    return jax.shard_map(
        update,
        mesh=grid,
        in_specs=(P(("x", "c"), ("y", "z")), P()),
        out_specs=P(("x", "c"), ("y", "z"), None, None),
        check_vma=False,
    )
```

```python
import functools

import jax
import jax.numpy as jnp
from jax import lax
from jax.experimental import pallas as pl
from jax.experimental.pallas import tpu as pltpu
from jax.sharding import Mesh
from jax.sharding import PartitionSpec as P


N = 4
VMEM = pltpu.VMEM
SMEM = pltpu.SMEM
GRANT = 16 * 1024 * 1024


def move(value, target):
    pairs = []
    for c in range(2):
        for y in range(N):
            for z in range(N):
                core, gather, scatter = target(c, *((y, z) if c else (z, y)))
                to = (gather, scatter) if c else (scatter, gather)
                pairs.append(((c * N + y) * N + z, (core * N + to[0] % N) * N + to[1] % N))
    return lax.ppermute(value, ("c", "y", "z"), pairs)


def along(value, step):
    return move(value, lambda c, g, r: (c, g + step, r))


def across(value, step):
    return move(value, lambda c, g, r: (c, g, r + step))


def along_other(value, step):
    return move(value, lambda c, g, r: (1 - c, g + step, r))


def swap(value):
    return lax.ppermute(value, "c", [(0, 1), (1, 0)])


def hop(value, pairs):
    return lax.ppermute(value, "x", pairs)


def specs(space, count):
    return [pl.BlockSpec(memory_space=space)] * count


def cut_kernel(q, group, at_ref, slab_ref, *refs):
    for step in range(N):
        part = lax.rem(at_ref[1] + step, N)
        for block in range(2):
            start = pl.multiple_of((2 * block + at_ref[0]) * N * q + part * q, q)
            row = (2 * group + block) * q
            refs[step - N][row : row + q, :] = slab_ref[pl.ds(start, q), :]


def cut(at, slab, held):
    rows, inner = slab.shape
    q = rows // 16
    return pl.pallas_call(
        functools.partial(cut_kernel, q, 1 if held else 0),
        out_shape=[jax.ShapeDtypeStruct((4 * q, inner), slab.dtype)] * N,
        in_specs=specs(SMEM, 1) + specs(VMEM, 1 + len(held)),
        out_specs=specs(VMEM, N),
        input_output_aliases={2 + k: k for k in range(len(held))},
        compiler_params=pltpu.CompilerParams(vmem_limit_bytes=GRANT),
        cost_estimate=pl.CostEstimate(flops=10**6, bytes_accessed=3 * rows * inner * 4, transcendentals=0),
        name="cut",
    )(at, slab, *held)


def product_kernel(q, work, carried, last, tab_ref, *refs):
    slabs = []
    for raw, places in work:
        a_refs, refs = refs[: 2 if raw else 1], refs[2 if raw else 1 :]
        slabs.append((raw, a_refs, list(zip(places, refs))))
        refs = refs[len(places) :]
    total_ref, refs = (refs[0], refs[1:]) if carried else (None, refs)
    raws = sum(raw for raw, _ in work)
    if last:
        outs, (acc, b_parts, *a_parts) = refs[:8], refs[8:]
    else:
        acc, a_parts, b_parts = refs[0], list(refs[1 : 1 + raws]), refs[-1]
    wide, side = 4 * q, 4 * q

    def halves(value, place, at):
        inner = value.shape[1]
        high = value.astype(jnp.bfloat16)
        place[at, :inner] = high
        place[at, inner:] = (value - high.astype(jnp.float32)).astype(jnp.bfloat16)

    terms = {}
    used = 0
    for raw, a_refs, pieces in slabs:
        if raw:
            parts = a_parts.pop(0)
            rows = a_refs[0].shape[0]
            for group in range(2):
                halves(a_refs[group][...], parts, slice(group * rows, (group + 1) * rows))
        else:
            parts = a_refs[0]
        for (place, row), ref in pieces:
            at = slice(wide * used, wide * (used + 1))
            halves(ref[row : row + wide, :], b_parts, at)
            terms.setdefault(place, []).append((parts, at))
            used += 1

    for n in range(8):
        columns = slice(n * side, (n + 1) * side)
        for place, pairs in terms.items():
            found = None
            for parts, at in pairs:
                inner = parts.shape[1] // 2
                for left, right in ((0, 0), (0, 1), (1, 0)):
                    one = lax.dot_general(
                        b_parts[at, left * inner : (left + 1) * inner],
                        parts[columns, right * inner : (right + 1) * inner],
                        (((1,), (1,)), ((), ())),
                        preferred_element_type=jnp.float32,
                    )
                    found = one if found is None else found + one
            rows = slice(wide * place, wide * (place + 1))
            if carried and place < 3:
                found = total_ref[n, rows, :] + found
            acc[n, rows, :] = found

    if last:
        for index in range(8):

            def place(k, carry, index=index):
                code = tab_ref[index * 8 + k]
                safe = jnp.maximum(code, 0)
                start = pl.multiple_of((safe // 2) * q, q)
                for b in range(2):
                    tile = acc[(index % 2) * 4 + (safe % 2) * 2 + b, pl.ds(start, q), :]
                    outs[index][k, :, b * side : (b + 1) * side] = jnp.where(code >= 0, tile, 0.0)
                return carry

            lax.fori_loop(0, 8, place, 0, unroll=4)


def product(tab, work, total, last):
    args, form, raws, used = [tab], [], 0, 0
    for rows, slices in work:
        args += list(rows) + [piece for piece, _ in slices.values()]
        raw = len(rows) == 2
        raws, used = raws + raw, used + len(slices)
        form.append((raw, tuple((place, row) for place, (_, row) in slices.items())))
    inner = work[0][1][0][0].shape[1] if 0 in work[0][1] else work[0][1][3][0].shape[1]
    wide = inner
    q, rows = wide // 4, 4 * wide
    if total is not None:
        args.append(total)
    parts = jax.ShapeDtypeStruct((2 * rows, 2 * inner), jnp.bfloat16)
    b_scratch = VMEM((wide * used, 2 * inner), jnp.bfloat16)
    if last:
        out_shape = [jax.ShapeDtypeStruct((8, q, rows // 2), jnp.float32)] * 8
        scratch = [VMEM((8, rows, wide), jnp.float32), b_scratch] + [VMEM(parts.shape, parts.dtype)] * raws
    else:
        out_shape = [jax.ShapeDtypeStruct((8, 3 * wide, wide), jnp.float32)] + [parts] * raws
        scratch = [b_scratch]
    return pl.pallas_call(
        functools.partial(product_kernel, q, form, total is not None, last),
        out_shape=out_shape,
        in_specs=specs(SMEM, 1) + specs(VMEM, len(args) - 1),
        out_specs=specs(VMEM, len(out_shape)),
        scratch_shapes=scratch,
        input_output_aliases={} if last or total is None else {len(args) - 1: 0},
        compiler_params=pltpu.CompilerParams(vmem_limit_bytes=GRANT),
        cost_estimate=pl.CostEstimate(
            flops=24 * rows * rows * inner, bytes_accessed=12 * rows * inner * 4, transcendentals=0
        ),
    )(*args)


def join_kernel(q, at_ref, *refs):
    pieces, out_ref, held = refs[:8], refs[8], refs[9]
    for index in range(8):
        kind = at_ref[0] if index < N else 1 - at_ref[0]
        mine = at_ref[1] if index < N else at_ref[2]
        part = lax.rem(mine + N - index % N, N)
        start = pl.multiple_of((kind * N + part) * q, q)
        for slot in range(2):
            held[slot, pl.ds(start, q), :] = pieces[index][slot]
    for slot in range(2):
        out_ref[0, slot] = held[slot].T


def join(at, pieces):
    _, q, half = pieces[0].shape
    return pl.pallas_call(
        functools.partial(join_kernel, q),
        out_shape=jax.ShapeDtypeStruct((1, 2, half, half), jnp.float32),
        in_specs=specs(SMEM, 1) + specs(VMEM, 8),
        out_specs=pl.BlockSpec(memory_space=VMEM),
        scratch_shapes=[VMEM((2, half, half), jnp.float32)],
        compiler_params=pltpu.CompilerParams(vmem_limit_bytes=GRANT),
        cost_estimate=pl.CostEstimate(flops=10**6, bytes_accessed=16 * half * half, transcendentals=0),
        name="join",
    )(at, *pieces)


def tile_codes(owner, x, c, gather, scatter):
    blocks = owner.shape[0]
    i = lax.broadcasted_iota(jnp.int32, (blocks, blocks), 0)
    j = lax.broadcasted_iota(jnp.int32, (blocks, blocks), 1)
    group = j // 2
    behind = (x - group // 2 + N) % N
    array = jnp.where(behind < 2, behind, 5 - behind) * 2 + jnp.where(group % 2 == c, 0, 1)
    code = jnp.where(j <= i, (array * 2 + j % 2) * 2 + i % 2 + 1, 0)
    index = jnp.arange(64, dtype=jnp.int32)
    far = (scatter + index // 16) % N
    mine = (index // 8) % 2
    near = (gather + (index // 2) % 4) % N
    wanted = jnp.where(c == 0, far * N + near, near * N + far) * 2 + index % 2
    wanted_group = 2 * x + jnp.where(mine == 0, c, 1 - c)
    hit = (owner[None] == wanted[:, None, None]) & ((i // 2)[None] == wanted_group[:, None, None])
    return jnp.sum(jnp.where(hit, code[None], 0), axis=(1, 2)) - 1


def update(panel, owner):
    x, c, y, z = (lax.axis_index(name) for name in "xcyz")
    gather, scatter = jnp.where(c == 0, z, y), jnp.where(c == 0, y, z)
    at = jnp.stack([c, gather, scatter]).astype(jnp.int32)
    tab = tile_codes(owner, x, c, gather, scatter)

    other = swap(panel)
    up, down = [along(panel, 1)], [along(panel, -1)]
    first, *sends = cut(at, other, cut(at, panel, []))
    small = [along(sends[s - 1], s) for s in range(1, N)]
    up.append(along(other, 1))
    down.append(along(other, -1))
    beyond = [along(up[0], 1), along(down[1], -1)]

    onward, wrap = [(0, 1), (1, 2), (2, 3)], [(0, 3)]
    both = jnp.concatenate([small[0], small[2]])
    a1, a3 = hop(first, onward), hop(first, wrap)
    b1, b3 = hop(both, onward), hop(both, wrap + [(1, 0)])
    c1, c3 = hop(small[1], onward), hop(small[1], wrap)
    a2, c2 = hop(a1, onward[1:]), hop(c1, onward[1:])
    b2 = hop(b3, wrap + [(3, 2)])

    wide = first.shape[0]
    low, high = [(v, 0) for v in (both, b1, b3, b2)], [(v, wide) for v in (both, b1, b3, b2)]
    zero, far = [(v, 0) for v in (first, a1, a3, a2)], [(v, 0) for v in (small[1], c1, c3, c2)]
    three, four = range(3), range(4)
    total, own_parts = product(tab, [((panel, other), dict(zip(three, zero)))], None, False)
    total, up_parts, down_parts = product(
        tab, [(up, dict(zip(three, low))), (down, dict(zip(three, high)))], total, False
    )
    outs = product(
        tab,
        [
            (beyond, dict(zip(four, far))),
            ((own_parts,), {3: zero[3]}),
            ((up_parts,), {3: low[3]}),
            ((down_parts,), {3: high[3]}),
        ],
        total,
        True,
    )
    own0, own1, near0, near1, far0, far1, last0, last1 = outs


    up_far, down_far = across(far0, 1), across(far1, -1)
    up_near, down_near = across(near1, 1), across(last0, -1)
    up_sum = across(near0 + up_far, 1)
    down_sum = across(last1 + down_far, -1)
    found, passed = [], []
    for s in range(N):
        part = slice(2 * s, 2 * s + 2)
        mine = own0[part] + up_sum[part] + down_near[part]
        theirs = own1[part] + down_sum[part] + up_near[part]
        found.append(mine if s == 0 else along(mine, s))
        passed.append(along_other(theirs, s))
    return join(at, found + passed)


def solution(mesh):
    grid = Mesh(mesh.devices.reshape(N, 2, N, N), ("x", "c", "y", "z"))
    return jax.shard_map(
        update,
        mesh=grid,
        in_specs=(P(("x", "c"), ("y", "z")), P()),
        out_specs=P(("x", "c"), ("y", "z"), None, None),
        check_vma=False,
    )
```

```python
import functools

import jax
import jax.numpy as jnp
from jax import lax
from jax.experimental import pallas as pl
from jax.experimental.pallas import tpu as pltpu
from jax.sharding import Mesh
from jax.sharding import PartitionSpec as P


N = 4
VMEM = pltpu.VMEM
SMEM = pltpu.SMEM
GRANT = 16 * 1024 * 1024


def move(value, target):
    pairs = []
    for c in range(2):
        for y in range(N):
            for z in range(N):
                core, gather, scatter = target(c, *((y, z) if c else (z, y)))
                to = (gather, scatter) if c else (scatter, gather)
                pairs.append(((c * N + y) * N + z, (core * N + to[0] % N) * N + to[1] % N))
    return lax.ppermute(value, ("c", "y", "z"), pairs)


def along(value, step):
    return move(value, lambda c, g, r: (c, g + step, r))


def across(value, step):
    return move(value, lambda c, g, r: (c, g, r + step))


def along_other(value, step):
    return move(value, lambda c, g, r: (1 - c, g + step, r))


def swap(value):
    return lax.ppermute(value, "c", [(0, 1), (1, 0)])


def hop(value, pairs):
    return lax.ppermute(value, "x", pairs)


def specs(space, count):
    return [pl.BlockSpec(memory_space=space)] * count


def cut_kernel(q, group, at_ref, slab_ref, *refs):
    for step in range(N):
        part = lax.rem(at_ref[1] + step, N)
        for block in range(2):
            start = pl.multiple_of((2 * block + at_ref[0]) * N * q + part * q, q)
            row = (2 * group + block) * q
            refs[step - N][row : row + q, :] = slab_ref[pl.ds(start, q), :]


def cut(at, slab, held):
    rows, inner = slab.shape
    q = rows // 16
    return pl.pallas_call(
        functools.partial(cut_kernel, q, 1 if held else 0),
        out_shape=[jax.ShapeDtypeStruct((4 * q, inner), slab.dtype)] * N,
        in_specs=specs(SMEM, 1) + specs(VMEM, 1 + len(held)),
        out_specs=specs(VMEM, N),
        input_output_aliases={2 + k: k for k in range(len(held))},
        compiler_params=pltpu.CompilerParams(vmem_limit_bytes=GRANT),
        cost_estimate=pl.CostEstimate(flops=10**6, bytes_accessed=3 * rows * inner * 4, transcendentals=0),
        name="cut",
    )(at, slab, *held)


def product_kernel(q, work, carried, groups, last, tab_ref, *refs):
    slabs = []
    for raw, places in work:
        count = len(groups) if raw else 1
        slabs.append((raw, refs[:count], list(zip(places, refs[count:]))))
        refs = refs[count + len(places) :]
    total_ref, refs = (refs[0], refs[1:]) if carried else (None, refs)
    raws = sum(raw for raw, _ in work)
    if last:
        (*outs, acc, b_parts, a_part), a_parts = refs, []
        a_parts.append(a_part)
    else:
        acc, a_parts, b_parts = refs[0], list(refs[1 : 1 + raws]), refs[-1]
    wide, side = 4 * q, 4 * q

    def halves(value, place, at):
        inner = value.shape[1]
        high = value.astype(jnp.bfloat16)
        place[at, :inner] = high
        place[at, inner:] = (value - high.astype(jnp.float32)).astype(jnp.bfloat16)

    terms = {}
    used = 0
    for raw, a_refs, pieces in slabs:
        if raw:
            parts, base = a_parts.pop(0), groups[0]
            rows = a_refs[0].shape[0]
            for k, ref in enumerate(a_refs):
                halves(ref[...], parts, slice(k * rows, (k + 1) * rows))
        else:
            parts, base = a_refs[0], 0
        for (place, row), ref in pieces:
            at = slice(wide * used, wide * (used + 1))
            halves(ref[row : row + wide, :], b_parts, at)
            terms.setdefault(place, []).append((parts, base, at))
            used += 1

    for n in range(4 * groups[0], 4 * groups[-1] + 4):
        to = n - 4 * groups[0] if last else n
        for place, pairs in terms.items():
            found = None
            for parts, base, at in pairs:
                inner = parts.shape[1] // 2
                column = (n - 4 * base) * side
                for left, right in ((0, 0), (0, 1), (1, 0)):
                    one = lax.dot_general(
                        b_parts[at, left * inner : (left + 1) * inner],
                        parts[column : column + side, right * inner : (right + 1) * inner],
                        (((1,), (1,)), ((), ())),
                        preferred_element_type=jnp.float32,
                    )
                    found = one if found is None else found + one
            rows = slice(wide * place, wide * (place + 1))
            if carried and place < 3:
                found = total_ref[n, rows, :] + found
            acc[to, rows, :] = found

    if last:
        offset = 0
        for ref in outs:
            first = (offset // 8 * 2 + groups[0]) * 8 + offset % 8

            def place(k, carry, ref=ref, first=first):
                code = tab_ref[first + k]
                safe = jnp.maximum(code, 0)
                start = pl.multiple_of((safe // 2) * q, q)
                for b in range(2):
                    tile = acc[(safe % 2) * 2 + b, pl.ds(start, q), :]
                    ref[k, :, b * side : (b + 1) * side] = jnp.where(code >= 0, tile, 0.0)
                return carry

            lax.fori_loop(0, ref.shape[0], place, 0, unroll=4)
            offset += ref.shape[0]


def product(tab, work, total, groups, sizes):
    args, form, raws, used = [tab], [], 0, 0
    for rows, slices in work:
        raw = rows[0].dtype == jnp.float32
        args += list(rows) + [piece for piece, _ in slices.values()]
        raws, used = raws + raw, used + len(slices)
        form.append((raw, tuple((place, row) for place, (_, row) in slices.items())))
    wide = next(iter(work[0][1].values()))[0].shape[1]
    q, rows, last = wide // 4, 4 * wide, bool(sizes)
    if total is not None:
        args.append(total)
    parts = (len(groups) * rows, 2 * wide)
    b_scratch = VMEM((wide * used, 2 * wide), jnp.bfloat16)
    if last:
        out_shape = [jax.ShapeDtypeStruct((k, q, rows // 2), jnp.float32) for k in sizes]
        scratch = [VMEM((4, rows, wide), jnp.float32), b_scratch, VMEM(parts, jnp.bfloat16)]
    else:
        out_shape = [jax.ShapeDtypeStruct((8, 3 * wide, wide), jnp.float32)]
        out_shape += [jax.ShapeDtypeStruct(parts, jnp.bfloat16)] * raws
        scratch = [b_scratch]
    return pl.pallas_call(
        functools.partial(product_kernel, q, form, total is not None, groups, last),
        out_shape=out_shape,
        in_specs=specs(SMEM, 1) + specs(VMEM, len(args) - 1),
        out_specs=specs(VMEM, len(out_shape)),
        scratch_shapes=scratch,
        input_output_aliases={} if last or total is None else {len(args) - 1: 0},
        compiler_params=pltpu.CompilerParams(vmem_limit_bytes=GRANT),
        cost_estimate=pl.CostEstimate(
            flops=12 * rows * rows * wide * len(groups), bytes_accessed=12 * rows * wide * 4, transcendentals=0
        ),
    )(*args)


def join_kernel(q, at_ref, *refs):
    pieces, out_ref, held = refs[:8], refs[8], refs[9]
    wide = held.shape[1]
    slot, columns = pl.program_id(0), pl.ds(pl.multiple_of(pl.program_id(1) * wide, wide), wide)
    for index in range(8):
        kind = at_ref[0] if index < N else 1 - at_ref[0]
        mine = at_ref[1] if index < N else at_ref[2]
        part = lax.rem(mine + N - index % N, N)
        start = pl.multiple_of((kind * N + part) * q, q)
        held[pl.ds(start, q), :] = pieces[index][slot, :, columns]
    out_ref[0, 0] = held[...].T


def join(at, pieces):
    _, q, half = pieces[0].shape
    wide = half // 2
    return pl.pallas_call(
        functools.partial(join_kernel, q),
        grid=(2, 2),
        out_shape=jax.ShapeDtypeStruct((1, 2, half, half), jnp.float32),
        in_specs=specs(SMEM, 1) + specs(VMEM, 8),
        out_specs=pl.BlockSpec((1, 1, wide, half), lambda slot, block: (0, slot, block, 0)),
        scratch_shapes=[VMEM((half, wide), jnp.float32)],
        compiler_params=pltpu.CompilerParams(vmem_limit_bytes=GRANT),
        cost_estimate=pl.CostEstimate(flops=10**6, bytes_accessed=16 * half * half, transcendentals=0),
        name="join",
    )(at, *pieces)


def tile_codes(owner, x, c, gather, scatter):
    blocks = owner.shape[0]
    i = lax.broadcasted_iota(jnp.int32, (blocks, blocks), 0)
    j = lax.broadcasted_iota(jnp.int32, (blocks, blocks), 1)
    group = j // 2
    behind = (x - group // 2 + N) % N
    array = jnp.where(behind < 2, behind, 5 - behind) * 2 + jnp.where(group % 2 == c, 0, 1)
    code = jnp.where(j <= i, (array * 2 + j % 2) * 2 + i % 2 + 1, 0)
    index = jnp.arange(64, dtype=jnp.int32)
    far = (scatter + index // 16) % N
    mine = (index // 8) % 2
    near = (gather + (index // 2) % 4) % N
    wanted = jnp.where(c == 0, far * N + near, near * N + far) * 2 + index % 2
    wanted_group = 2 * x + jnp.where(mine == 0, c, 1 - c)
    hit = (owner[None] == wanted[:, None, None]) & ((i // 2)[None] == wanted_group[:, None, None])
    return jnp.sum(jnp.where(hit, code[None], 0), axis=(1, 2)) - 1


def update(panel, owner):
    x, c, y, z = (lax.axis_index(name) for name in "xcyz")
    gather, scatter = jnp.where(c == 0, z, y), jnp.where(c == 0, y, z)
    at = jnp.stack([c, gather, scatter]).astype(jnp.int32)
    tab = tile_codes(owner, x, c, gather, scatter)

    other = swap(panel)
    up, down = [along(panel, 1)], [along(panel, -1)]
    first, *sends = cut(at, other, cut(at, panel, []))
    small = [along(sends[s - 1], s) for s in range(1, N)]
    up.append(along(other, 1))
    down.append(along(other, -1))
    beyond = [along(up[0], 1), along(down[1], -1)]

    onward, wrap = [(0, 1), (1, 2), (2, 3)], [(0, 3)]
    both = jnp.concatenate([small[0], small[2]])
    a1, a3 = hop(first, onward), hop(first, wrap)
    b1, b3 = hop(both, onward), hop(both, wrap + [(1, 0)])
    c1, c3 = hop(small[1], onward), hop(small[1], wrap)
    a2, c2 = hop(a1, onward[1:]), hop(c1, onward[1:])
    b2 = hop(b3, wrap + [(3, 2)])

    wide = first.shape[0]
    low, high = [(v, 0) for v in (both, b1, b3, b2)], [(v, wide) for v in (both, b1, b3, b2)]
    zero, far = [(v, 0) for v in (first, a1, a3, a2)], [(v, 0) for v in (small[1], c1, c3, c2)]
    three, four = range(3), range(4)
    total, own_parts = product(tab, [((panel, other), dict(zip(three, zero)))], None, (0, 1), ())
    total, up_parts, down_parts = product(
        tab, [(up, dict(zip(three, low))), (down, dict(zip(three, high)))], total, (0, 1), ()
    )
    rest = [((own_parts,), {3: zero[3]}), ((up_parts,), {3: low[3]}), ((down_parts,), {3: high[3]})]
    own0, near0, far0, last0 = product(tab, [((beyond[0],), dict(zip(four, far)))] + rest, total, (0,), (8, 8, 8, 8))
    up_far, down_near = across(far0, 1), across(last0, -1)
    own1, near1, near1b, far1, last1 = product(
        tab, [((beyond[1],), dict(zip(four, far)))] + rest, total, (1,), (8, 4, 4, 8, 8)
    )
    down_far = across(far1, -1)
    up_near = across(near1, 1)
    up_sum = across(near0 + up_far, 1)
    up_near = [up_near, across(near1b, 1)]
    down_sum = across(last1 + down_far, -1)

    found, passed = [], []
    for s in range(N):
        part, piece = slice(2 * s, 2 * s + 2), slice(2 * (s % 2), 2 * (s % 2) + 2)
        mine = own0[part] + up_sum[part] + down_near[part]
        theirs = own1[part] + down_sum[part] + up_near[s // 2][piece]
        found.append(mine if s == 0 else along(mine, s))
        passed.append(along_other(theirs, s))
    return join(at, found + passed)


def solution(mesh):
    grid = Mesh(mesh.devices.reshape(N, 2, N, N), ("x", "c", "y", "z"))
    return jax.shard_map(
        update,
        mesh=grid,
        in_specs=(P(("x", "c"), ("y", "z")), P()),
        out_specs=P(("x", "c"), ("y", "z"), None, None),
        check_vma=False,
    )
```

```python
import functools

import jax
import jax.numpy as jnp
from jax import lax
from jax.experimental import pallas as pl
from jax.experimental.pallas import tpu as pltpu
from jax.sharding import Mesh
from jax.sharding import PartitionSpec as P


N = 4
VMEM = pltpu.VMEM
SMEM = pltpu.SMEM
GRANT = 16 * 1024 * 1024


def move(value, target):
    pairs = []
    for c in range(2):
        for y in range(N):
            for z in range(N):
                core, gather, scatter = target(c, *((y, z) if c else (z, y)))
                to = (gather, scatter) if c else (scatter, gather)
                pairs.append(((c * N + y) * N + z, (core * N + to[0] % N) * N + to[1] % N))
    return lax.ppermute(value, ("c", "y", "z"), pairs)


def along(value, step):
    return move(value, lambda c, g, r: (c, g + step, r))


def across(value, step):
    return move(value, lambda c, g, r: (c, g, r + step))


def along_other(value, step):
    return move(value, lambda c, g, r: (1 - c, g + step, r))


def swap(value):
    return lax.ppermute(value, "c", [(0, 1), (1, 0)])


def hop(value, pairs):
    return lax.ppermute(value, "x", pairs)


def specs(space, count):
    return [pl.BlockSpec(memory_space=space)] * count


def cut_kernel(q, group, at_ref, slab_ref, *refs):
    for step in range(N):
        part = lax.rem(at_ref[1] + step, N)
        for block in range(2):
            start = pl.multiple_of((2 * block + at_ref[0]) * N * q + part * q, q)
            row = (2 * group + block) * q
            refs[step - N][row : row + q, :] = slab_ref[pl.ds(start, q), :]


def cut(at, slab, held):
    rows, inner = slab.shape
    q = rows // 16
    return pl.pallas_call(
        functools.partial(cut_kernel, q, 1 if held else 0),
        out_shape=[jax.ShapeDtypeStruct((4 * q, inner), slab.dtype)] * N,
        in_specs=specs(SMEM, 1) + specs(VMEM, 1 + len(held)),
        out_specs=specs(VMEM, N),
        input_output_aliases={2 + k: k for k in range(len(held))},
        compiler_params=pltpu.CompilerParams(vmem_limit_bytes=GRANT),
        cost_estimate=pl.CostEstimate(flops=10**6, bytes_accessed=3 * rows * inner * 4, transcendentals=0),
        name="cut",
    )(at, slab, *held)


def product_kernel(q, work, carried, groups, last, tab_ref, *refs):
    slabs = []
    for raw, places in work:
        count = len(groups) if raw else 1
        slabs.append((raw, refs[:count], list(zip(places, refs[count:]))))
        refs = refs[count + len(places) :]
    total_ref, refs = (refs[0], refs[1:]) if carried else (None, refs)
    raws = sum(raw for raw, _ in work)
    if last:
        (*outs, acc, b_parts, a_part), a_parts = refs, []
        a_parts.append(a_part)
    else:
        acc, a_parts, b_parts = refs[0], list(refs[1 : 1 + raws]), refs[-1]
    wide, side = 4 * q, 4 * q

    def halves(value, place, at):
        inner = value.shape[1]
        high = value.astype(jnp.bfloat16)
        place[at, :inner] = high
        place[at, inner:] = (value - high.astype(jnp.float32)).astype(jnp.bfloat16)

    terms = {}
    used = 0
    for raw, a_refs, pieces in slabs:
        if raw:
            parts, base = a_parts.pop(0), groups[0]
            rows = a_refs[0].shape[0]
            for k, ref in enumerate(a_refs):
                halves(ref[...], parts, slice(k * rows, (k + 1) * rows))
        else:
            parts, base = a_refs[0], 0
        for (place, row), ref in pieces:
            at = slice(wide * used, wide * (used + 1))
            halves(ref[row : row + wide, :], b_parts, at)
            terms.setdefault(place, []).append((parts, base, at))
            used += 1

    for n in range(4 * groups[0], 4 * groups[-1] + 4):
        to = n - 4 * groups[0] if last else n
        for place, pairs in terms.items():
            found = None
            for parts, base, at in pairs:
                inner = parts.shape[1] // 2
                column = (n - 4 * base) * side
                for left, right in ((0, 0), (0, 1), (1, 0)):
                    one = lax.dot_general(
                        b_parts[at, left * inner : (left + 1) * inner],
                        parts[column : column + side, right * inner : (right + 1) * inner],
                        (((1,), (1,)), ((), ())),
                        preferred_element_type=jnp.float32,
                    )
                    found = one if found is None else found + one
            rows = slice(wide * place, wide * (place + 1))
            if carried and place < 3:
                found = total_ref[n, rows, :] + found
            acc[to, rows, :] = found

    if last:
        offset = 0
        for ref in outs:
            first = (offset // 8 * 2 + groups[0]) * 8 + offset % 8

            def place(k, carry, ref=ref, first=first):
                code = tab_ref[first + k]
                safe = jnp.maximum(code, 0)
                start = pl.multiple_of((safe // 2) * q, q)
                for b in range(2):
                    tile = acc[(safe % 2) * 2 + b, pl.ds(start, q), :]
                    ref[k, :, b * side : (b + 1) * side] = jnp.where(code >= 0, tile, 0.0)
                return carry

            lax.fori_loop(0, ref.shape[0], place, 0, unroll=4)
            offset += ref.shape[0]


def product(tab, work, total, groups, sizes):
    args, form, raws, used = [tab], [], 0, 0
    for rows, slices in work:
        raw = rows[0].dtype == jnp.float32
        args += list(rows) + [piece for piece, _ in slices.values()]
        raws, used = raws + raw, used + len(slices)
        form.append((raw, tuple((place, row) for place, (_, row) in slices.items())))
    wide = next(iter(work[0][1].values()))[0].shape[1]
    q, rows, last = wide // 4, 4 * wide, bool(sizes)
    if total is not None:
        args.append(total)
    parts = (len(groups) * rows, 2 * wide)
    b_scratch = VMEM((wide * used, 2 * wide), jnp.bfloat16)
    if last:
        out_shape = [jax.ShapeDtypeStruct((k, q, rows // 2), jnp.float32) for k in sizes]
        scratch = [VMEM((4, rows, wide), jnp.float32), b_scratch, VMEM(parts, jnp.bfloat16)]
    else:
        out_shape = [jax.ShapeDtypeStruct((8, 3 * wide, wide), jnp.float32)]
        out_shape += [jax.ShapeDtypeStruct(parts, jnp.bfloat16)] * raws
        scratch = [b_scratch]
    return pl.pallas_call(
        functools.partial(product_kernel, q, form, total is not None, groups, last),
        out_shape=out_shape,
        in_specs=specs(SMEM, 1) + specs(VMEM, len(args) - 1),
        out_specs=specs(VMEM, len(out_shape)),
        scratch_shapes=scratch,
        input_output_aliases={} if last or total is None else {len(args) - 1: 0},
        compiler_params=pltpu.CompilerParams(vmem_limit_bytes=GRANT),
        cost_estimate=pl.CostEstimate(
            flops=12 * rows * rows * wide * len(groups), bytes_accessed=12 * rows * wide * 4, transcendentals=0
        ),
    )(*args)


def join_kernel(q, at_ref, *refs):
    pieces, out_ref, held = refs[:8], refs[8], refs[9]
    for index in range(8):
        kind = at_ref[0] if index < N else 1 - at_ref[0]
        mine = at_ref[1] if index < N else at_ref[2]
        part = lax.rem(mine + N - index % N, N)
        start = pl.multiple_of((kind * N + part) * q, q)
        for slot in range(2):
            held[slot, pl.ds(start, q), :] = pieces[index][slot]
    for slot in range(2):
        out_ref[0, slot] = held[slot].T


def join(at, pieces):
    _, q, half = pieces[0].shape
    return pl.pallas_call(
        functools.partial(join_kernel, q),
        out_shape=jax.ShapeDtypeStruct((1, 2, half, half), jnp.float32),
        in_specs=specs(SMEM, 1) + specs(VMEM, 8),
        out_specs=pl.BlockSpec(memory_space=VMEM),
        scratch_shapes=[VMEM((2, half, half), jnp.float32)],
        compiler_params=pltpu.CompilerParams(vmem_limit_bytes=GRANT),
        cost_estimate=pl.CostEstimate(flops=10**6, bytes_accessed=16 * half * half, transcendentals=0),
        name="join",
    )(at, *pieces)


def tile_codes(owner, x, c, gather, scatter):
    blocks = owner.shape[0]
    i = lax.broadcasted_iota(jnp.int32, (blocks, blocks), 0)
    j = lax.broadcasted_iota(jnp.int32, (blocks, blocks), 1)
    group = j // 2
    behind = (x - group // 2 + N) % N
    array = jnp.where(behind < 2, behind, 5 - behind) * 2 + jnp.where(group % 2 == c, 0, 1)
    code = jnp.where(j <= i, (array * 2 + j % 2) * 2 + i % 2 + 1, 0)
    index = jnp.arange(64, dtype=jnp.int32)
    far = (scatter + index // 16) % N
    mine = (index // 8) % 2
    near = (gather + (index // 2) % 4) % N
    wanted = jnp.where(c == 0, far * N + near, near * N + far) * 2 + index % 2
    wanted_group = 2 * x + jnp.where(mine == 0, c, 1 - c)
    hit = (owner[None] == wanted[:, None, None]) & ((i // 2)[None] == wanted_group[:, None, None])
    return jnp.sum(jnp.where(hit, code[None], 0), axis=(1, 2)) - 1


def update(panel, owner):
    x, c, y, z = (lax.axis_index(name) for name in "xcyz")
    gather, scatter = jnp.where(c == 0, z, y), jnp.where(c == 0, y, z)
    at = jnp.stack([c, gather, scatter]).astype(jnp.int32)
    tab = tile_codes(owner, x, c, gather, scatter)

    other = swap(panel)
    up, down = [along(panel, 1)], [along(panel, -1)]
    first, *sends = cut(at, other, cut(at, panel, []))
    small = [along(sends[s - 1], s) for s in range(1, N)]
    up.append(along(other, 1))
    down.append(along(other, -1))
    beyond = [along(up[0], 1), along(down[1], -1)]

    onward, wrap = [(0, 1), (1, 2), (2, 3)], [(0, 3)]
    both = jnp.concatenate([small[0], small[2]])
    a1, a3 = hop(first, onward), hop(first, wrap)
    b1, b3 = hop(both, onward), hop(both, wrap + [(1, 0)])
    c1, c3 = hop(small[1], onward), hop(small[1], wrap)
    a2, c2 = hop(a1, onward[1:]), hop(c1, onward[1:])
    b2 = hop(b3, wrap + [(3, 2)])

    wide = first.shape[0]
    low, high = [(v, 0) for v in (both, b1, b3, b2)], [(v, wide) for v in (both, b1, b3, b2)]
    zero, far = [(v, 0) for v in (first, a1, a3, a2)], [(v, 0) for v in (small[1], c1, c3, c2)]
    three, four = range(3), range(4)
    total, own_parts = product(tab, [((panel, other), dict(zip(three, zero)))], None, (0, 1), ())
    total, up_parts, down_parts = product(
        tab, [(up, dict(zip(three, low))), (down, dict(zip(three, high)))], total, (0, 1), ()
    )
    rest = [((own_parts,), {3: zero[3]}), ((up_parts,), {3: low[3]}), ((down_parts,), {3: high[3]})]
    own0, near0, far0, last0 = product(tab, [((beyond[0],), dict(zip(four, far)))] + rest, total, (0,), (8, 8, 8, 8))
    up_far, down_near = across(far0, 1), across(last0, -1)
    own1, near1, near1b, far1, last1 = product(
        tab, [((beyond[1],), dict(zip(four, far)))] + rest, total, (1,), (8, 4, 4, 8, 8)
    )
    down_far = across(far1, -1)
    up_near = across(near1, 1)
    up_sum = across(near0 + up_far, 1)
    up_near = [up_near, across(near1b, 1)]
    down_sum = across(last1 + down_far, -1)

    found, passed = [], []
    for s in range(N):
        part, piece = slice(2 * s, 2 * s + 2), slice(2 * (s % 2), 2 * (s % 2) + 2)
        mine = own0[part] + up_sum[part] + down_near[part]
        theirs = own1[part] + down_sum[part] + up_near[s // 2][piece]
        found.append(mine if s == 0 else along(mine, s))
        passed.append(along_other(theirs, s))
    return join(at, found + passed)


def solution(mesh):
    grid = Mesh(mesh.devices.reshape(N, 2, N, N), ("x", "c", "y", "z"))
    return jax.shard_map(
        update,
        mesh=grid,
        in_specs=(P(("x", "c"), ("y", "z")), P()),
        out_specs=P(("x", "c"), ("y", "z"), None, None),
        check_vma=False,
    )
```
